32 devices in a mesh: dp: 2 (over z, core), tp: 16 (over x, y).
Axes of the slice: x: 4, y: 4, z: 1, core: 2. Of those that a mesh axis runs over, the one named last changes fastest.
The devices are a block of a 4x4x8 slice.
Arguments:
- x: bfloat16 [4096, 14336], P(('dp', 'tp')), parts along dimension 0
- gain: bfloat16 [14336], replicated
- wq: bfloat16 [14336, 14336], P(None, 'tp')
- wk: bfloat16 [14336, 14336], P(None, 'tp')
- wv: bfloat16 [14336, 14336], P(None, 'tp')
- wo: bfloat16 [14336, 14336], P('tp')
Outputs:
- output: bfloat16 [4096, 14336], P(('dp', 'tp')), parts along dimension 0
There are 2 independent parts. The reference program is written for one: setup_inputs(seed, part) draws one part's arguments, and reference() takes and returns one part's arrays. A program takes and returns all parts, laid end to end along the dimension named above; an argument that names none is the same for every part.
All inputs are finite; a program needn't handle non-finite values.
Results may differ from the reference program's by a relative error of at most 0.012.
Values are sent between devices in bfloat16 or wider.
A program may use at most 768 MiB of HBM per device.

```python
import jax
import jax.numpy as jnp
from jax import lax

ROWS = 2048
D = 14336
HEADS = 112
KV_HEADS = 112
HEAD = 128
THETA = 10000


def setup_inputs(seed: int = 0, part: int = 0) -> dict:
    kx, kn, kq, kk, kv, ko = jax.random.split(jax.random.key(seed), 6)

    def weights(key, rows, columns):
        return jax.random.normal(key, (rows, columns), jnp.float32) * rows**-0.5

    drawn = {
        "x": jax.random.normal(jax.random.fold_in(kx, part), (ROWS, D), jnp.float32),
        "gain": 1 + 0.1 * jax.random.normal(kn, (D,), jnp.float32),
        "wq": 2 * weights(kq, D, HEADS * HEAD),
        "wk": 2 * weights(kk, D, KV_HEADS * HEAD),
        "wv": 4 * weights(kv, D, KV_HEADS * HEAD),
        "wo": weights(ko, HEADS * HEAD, D),
    }
    return {k: v.astype(jnp.bfloat16) for k, v in drawn.items()}


def normed(x, gain):
    wide = x.astype(jnp.float32)
    scale = lax.rsqrt(jnp.mean(wide * wide, -1, keepdims=True) + 1e-6)
    return (wide * scale * gain.astype(jnp.float32)).astype(jnp.bfloat16)


def turned(t, place, theta):
    half = t.shape[-1] // 2
    angle = place.astype(jnp.float32)[:, None] * theta ** (-jnp.arange(half, dtype=jnp.float32) / half)
    cos, sin = jnp.cos(angle)[:, None], jnp.sin(angle)[:, None]
    a, b = t[..., :half].astype(jnp.float32), t[..., half:].astype(jnp.float32)
    return jnp.concatenate([a * cos - b * sin, b * cos + a * sin], -1).astype(jnp.bfloat16)


def matmul(a, w):
    return jnp.dot(a, w, preferred_element_type=jnp.float32).astype(jnp.bfloat16)


def einsum(form, a, b):
    return jnp.einsum(form, a.astype(jnp.float32), b.astype(jnp.float32))


def attention(q, k, v):
    scores = einsum("tgsd,ugd->gstu", q, k) * q.shape[-1] ** -0.5
    token = jnp.arange(q.shape[0])
    scores = jnp.where(token[:, None] >= token, scores, -jnp.inf)
    weights = jax.nn.softmax(scores, -1).astype(jnp.bfloat16)
    return einsum("gstu,ugd->tgsd", weights, v).astype(jnp.bfloat16)


def reference(x, gain, wq, wk, wv, wo):
    a, place = normed(x, gain), jnp.arange(ROWS)
    q = turned(matmul(a, wq).reshape(ROWS, HEADS, HEAD), place, THETA).reshape(ROWS, KV_HEADS, -1, HEAD)
    k = turned(matmul(a, wk).reshape(ROWS, KV_HEADS, HEAD), place, THETA)
    v = matmul(a, wv).reshape(ROWS, KV_HEADS, HEAD)
    seen = attention(q, k, v).reshape(ROWS, HEADS * HEAD)
    return (x.astype(jnp.float32) + jnp.dot(seen, wo, preferred_element_type=jnp.float32)).astype(jnp.bfloat16)
```

```python
import functools
import heapq

import jax
import jax.numpy as jnp
import numpy as np
from jax import lax
from jax.experimental import pallas as pl
from jax.experimental.pallas import tpu as pltpu
from jax.sharding import PartitionSpec as P

NEG = -1e30
HIDDEN = 2 * NEG
LOG2E = 1.4426950408889634
HEAD = 128
HALF = HEAD // 2
THETA = 10000
EPSILON = 1e-6
VMEM = 62 * 2**20
MESH = pl.DeviceIdType.MESH
ANYWHERE = pl.BlockSpec(memory_space=pl.ANY)
NEAR = pl.BlockSpec(memory_space=pltpu.VMEM)
LOW, WIDE = jnp.bfloat16, jnp.float32
DMA = pltpu.SemaphoreType.DMA
BOTH = (0, 1)


def fit(size, want):
    return max(n for n in range(HEAD, max(min(want, size), HEAD) + 1, HEAD) if size % n == 0)


def dot(a, b, ca, cb):
    return lax.dot_general(a, b, (((ca,), (cb,)), ((), ())), preferred_element_type=WIDE)


BLOCK = 512


def attention_kernel(q_ref, k_ref, v_ref, o_ref, top_s, mix_s, gap_s):
    heads, bq, d = q_ref.shape
    iq = pl.program_id(0)
    e = d**-0.5 * LOG2E
    gap_s[...] = lax.broadcasted_iota(jnp.int32, (bq, bq), 1) - lax.broadcasted_iota(jnp.int32, (bq, bq), 0)
    for h in range(heads):
        top_s[h : h + 1, :] = jnp.full((1, bq), NEG, WIDE)
        mix_s[h] = jnp.zeros(mix_s.shape[1:], WIDE)
    ones = jnp.ones((mix_s.shape[1] - d, bq), LOW)

    def block(j, masked):
        here = pl.ds(pl.multiple_of(j * bq, bq), bq)
        scores = [dot(k_ref[h, here, :], q_ref[h], 1, 1) for h in range(heads)]
        weights, keeps = [], []
        for h, s in enumerate(scores):
            if masked:
                s = jnp.where(gap_s[...] >= 0, s, HIDDEN)
            old = top_s[h : h + 1, :]
            top = jnp.maximum(old, s.max(axis=0, keepdims=True))
            top_s[h : h + 1, :] = top
            weights.append(jnp.exp2((s - top) * e).astype(LOW))
            keeps.append(jnp.exp2((old - top) * e))
        for h, (p, keep) in enumerate(zip(weights, keeps)):
            values = jnp.concatenate([v_ref[h, here, :].T, ones], axis=0)
            mix_s[h] = mix_s[h] * keep + dot(values, p, 1, 0)

    lax.fori_loop(0, iq, lambda j, _: block(j, False), None)
    block(iq, True)
    for h in range(heads):
        o_ref[h] = (mix_s[h, :d, :] * (1 / mix_s[h, d : d + 1, :])).T.astype(o_ref.dtype)


def attend(q, k, v):
    heads, tokens, d = q.shape
    bq = fit(tokens, BLOCK)
    some = pl.BlockSpec((heads, bq, d), lambda i: (0, i, 0))
    return pl.pallas_call(
        attention_kernel,
        grid=(tokens // bq,),
        in_specs=[some, NEAR, NEAR],
        out_specs=some,
        out_shape=jax.ShapeDtypeStruct(q.shape, q.dtype),
        scratch_shapes=[pltpu.VMEM((heads, bq), WIDE), pltpu.VMEM((heads, d + 8, bq), WIDE), pltpu.VMEM((bq, bq), jnp.int32)],
        compiler_params=pltpu.CompilerParams(dimension_semantics=("arbitrary",), vmem_limit_bytes=VMEM),
        cost_estimate=pl.CostEstimate(flops=4 * q.size * tokens, transcendentals=heads * tokens**2, bytes_accessed=8 * q.size),
        name="attention",
    )(q, k, v)


SIDE = 4
PIECES = 4
LUMP = 1
TURN = 12
KINDS = 48


def plan_gather(tiles, tile_us):
    free, queue, done, groups = {}, [], [0] * PIECES, [[]]
    rate, delay = PIECES * 0.051, 2.5

    def send(t, m):
        stage, _, path, kind, sign, half = m
        link = (path if stage == 1 else 1 - path, sign)
        size = (1 if kind < 3 or stage == 1 else 0.5) * (0.5 if half else 1)
        free[link] = max(t, free.get(link, 0)) + size / rate
        heapq.heappush(queue, (free[link] + delay, len(queue), len(groups), m))
        groups[-1].append(("send", m))

    def begin(piece, t):
        for path in BOTH:
            for stage in (1, 2):
                for sign in (1, -1):
                    send(t, (stage, piece, path, 0, sign, 0))

    begun, t, tile, loaded = 1, 0, 0, 0
    begin(0, t)
    while queue or tile < tiles * PIECES // LUMP:
        while queue and queue[0][0] <= t:
            m = heapq.heappop(queue)[-1]
            groups[-1].append(("wait", m))
            stage, piece, path, kind, sign, half = m
            if stage == 1:
                if not half:
                    send(t, (1, piece, path, 0, sign, 1))
                kind = (1 if sign == 1 else 2) + 2 * half
                for way in (1, -1):
                    send(t, (2, piece, path, kind, way, 0))
            elif not half:
                send(t, (2, piece, path, kind, sign, 1))
            done[piece] += 1
            if begun < PIECES and done[begun - 1] * 3 >= KINDS:
                begin(begun, t)
                begun += 1
        while loaded * LUMP < PIECES and done[loaded * LUMP + LUMP - 1] == done[loaded * LUMP] == KINDS and tile >= (loaded - 1) * tiles:
            groups[-1].append(("load", loaded))
            loaded += 1
        if tile // tiles < loaded:
            groups.append([])
            tile += 1
            t += tile_us
        elif queue:
            t = max(t, queue[0][0])
    return groups


def place_in(t):
    pos = (lax.div(t, SIDE), lax.rem(t, SIDE))

    def at(path, da, db):
        a, b = lax.rem(pos[path] + da + SIDE, SIDE), lax.rem(pos[1 - path] + db + SIDE, SIDE)
        return a * SIDE + b if path == 0 else b * SIDE + a

    return pos, at


def greet(devices):
    barrier = pltpu.get_barrier_semaphore()
    for device in devices:
        pl.semaphore_signal(barrier, 1, device_id=device, device_id_type=MESH)
    return lambda: pl.semaphore_wait(barrier, len(devices))


def gather_kernel(plan, x_ref, gain_ref, freq_ref, wq, wk, wv, xg, q, k, v, xb, wb, ob, acc, cos, sin, bsem, lsem, xsem, wsem, osem, ssem, rsem, turn):
    owners, tokens, dim = xg.shape
    rows = tokens // PIECES
    lump = rows * LUMP
    m_rows = owners * lump
    split = dim // 2
    heads = q.shape[0]
    t = lax.axis_index("tp")
    pair = lax.axis_index("dp")
    second = lax.rem(pair, 2)
    other = {"dp": pair + 1 - 2 * second, "tp": t}
    _, at = place_in(t)

    def block(m, sending):
        stage, piece, path, kind, sign, half = m
        da, db, lo, width = 0, 0, 0, 4
        if stage == 1:
            da = -sign * half
            if half:
                width = 2
                lo = 1 - sign
        else:
            da, db = (0, -1, 1, 2, 2)[kind], -sign * half
            if kind > 2:
                width = 2
                lo = 2 * (kind - 3)
            if half:
                width //= 2
                lo += 0 if sign == 1 else width
        if not sending:
            da, db = (da - sign, db) if stage == 1 else (da, db - sign)
        return xg.at[at(path, da, db), pl.ds(piece * rows, rows), pl.ds(path * split + lo * split // 4, width * split // 4)]

    def message(m, sending):
        stage, piece, path, kind, sign, half = m
        key = (stage - 1) * 8 + path * 4 + kind * 8 + (sign + 1) // 2 + 2 * half
        here = block(m, sending)
        to = (at(path, sign, 0) if stage == 1 else at(path, 0, sign)) if sending else t
        return pltpu.make_async_remote_copy(here, here, ssem, rsem.at[piece, key], device_id={"tp": to}, device_id_type=MESH)

    given = ((wq, q), (wk, k), (wv, v))
    arrays = range(len(given))
    even = heads - heads % 2
    units = [(a, h) for a in arrays for h in range(even)] + [(a, h) for h in range(even, heads) for a in arrays]
    tiles = [units[n : n + 2] for n in range(0, len(units), 2)]
    nt = len(tiles)
    steps = nt * PIECES // LUMP

    def weights(j, slot):
        for n, tile in enumerate(tiles):

            @pl.when(j == n)
            def _(tile=tile):
                (a, h), (b, _) = tile[0], tile[-1]
                if a == b and len(tile) == 2:
                    pltpu.make_async_copy(given[a][0].at[:, pl.ds(h * HEAD, 2 * HEAD)], wb.at[slot], wsem.at[slot]).start()
                else:
                    for i, (a, h) in enumerate(tile):
                        pltpu.make_async_copy(given[a][0].at[:, pl.ds(h * HEAD, HEAD)], wb.at[slot, :, pl.ds(i * HEAD, HEAD)], wsem.at[slot]).start()

    def weights_wait(j, slot):
        @pl.when(j < nt - 1)
        def _():
            pltpu.make_async_copy(wb.at[slot], wb.at[slot], wsem.at[slot]).wait()

        @pl.when(j == nt - 1)
        def _():
            part = wb.at[slot, :, pl.ds(0, len(tiles[-1]) * HEAD)]
            pltpu.make_async_copy(part, part, wsem.at[slot]).wait()

    def results(i, start):
        c, j, slot = lax.div(i, nt), lax.rem(i, nt), lax.rem(i, 2)
        for n, tile in enumerate(tiles):

            @pl.when(j == n)
            def _(tile=tile):
                for i, (a, h) in enumerate(tile):
                    copy = pltpu.make_async_copy(ob.at[slot, i], given[a][1].at[h, :, pl.ds(pl.multiple_of(c * lump, lump), lump), :], osem.at[slot, i])
                    copy.start() if start else copy.wait()

    def finish(i):
        c, j, slot = lax.div(i, nt), lax.rem(i, nt), lax.rem(i, 2)
        here = pl.ds(pl.multiple_of(c * lump, lump), lump)
        turns = functools.reduce(lambda a, b: a | b, [j == n for n, tile in enumerate(tiles) if tile[0][0] < 2])

        @pl.when(turns)
        def _():
            co, si = cos[:, here, :].reshape(m_rows, HEAD), sin[:, here, :].reshape(m_rows, HEAD)
            for n in BOTH:
                plain = acc[:, n * HEAD : (n + 1) * HEAD].astype(LOW).astype(WIDE)
                ob[slot, n] = (plain * co + pltpu.roll(plain, HALF, 1) * si).astype(LOW).reshape(owners, lump, HEAD)

        @pl.when(~turns)
        def _():
            for n in BOTH:
                ob[slot, n] = acc[:, n * HEAD : (n + 1) * HEAD].astype(LOW).reshape(owners, lump, HEAD)

    def load(c):
        return pltpu.make_async_copy(xg.at[:, pl.ds(c * lump, lump), :], xb.at[c % 2], xsem.at[c % 2])

    def actions(group):
        for what, m in group:
            if what == "send":
                message(m, True).start()
            elif what == "wait":
                message(m, False).wait_recv()
            elif what == "load":
                load(m).start()
            else:

                @pl.when(second == 0)
                def _():
                    pl.semaphore_signal(turn, 1, device_id=other, device_id_type=MESH)

    per = lump // rows

    def staged(n):
        return xb.at[1, n // per, pl.ds(n % per * rows, rows)]

    def raw(c):
        return pltpu.make_async_copy(x_ref.at[pl.ds(c * rows, rows), :], staged(c), lsem.at[c])

    def own(c):
        return pltpu.make_async_copy(staged(PIECES + c), xg.at[t, pl.ds(c * rows, rows), :], bsem.at[c])

    wide = fit(dim, 1024)

    def norm(c):
        raw(c).wait()
        src, dst = staged(c), staged(PIECES + c)

        def square(n, total):
            part = src[:, pl.ds(pl.multiple_of(n * wide, wide), wide)].astype(WIDE)
            return total + part * part

        total = lax.fori_loop(0, dim // wide, square, jnp.zeros((rows, wide), WIDE))
        scale = lax.rsqrt(jnp.sum(total, -1, keepdims=True) * (1 / dim) + EPSILON)

        def scaled(n, _):
            here = pl.ds(pl.multiple_of(n * wide, wide), wide)
            dst[:, here] = (src[:, here].astype(WIDE) * scale * gain_ref[here].astype(WIDE)[None]).astype(LOW)
            return 0

        lax.fori_loop(0, dim // wide, scaled, 0)
        own(c).start()

    for c in range(PIECES):
        raw(c).start()
    met = greet([{"tp": near} for near in (at(0, 1, 0), at(0, -1, 0), at(0, 0, 1), at(0, 0, -1))] + [other])
    weights(0, 0)
    norm(0)
    met()

    @pl.when(second == 1)
    def _():
        for c in range(1, PIECES):
            norm(c)
        pl.semaphore_wait(turn, 1)

    own(0).wait()
    first = [n for n, (what, _) in enumerate(plan[0]) if what == "wait"][0]
    actions(plan[0][:first])

    @pl.when(second == 0)
    def _():
        for c in range(1, PIECES):
            norm(c)

    for c in range(1, PIECES):
        own(c).wait()

    def table(n, _):
        place = (lax.broadcasted_iota(jnp.int32, (tokens, HEAD), 0) + n * tokens).astype(WIDE)
        angle = place * jnp.abs(freq_ref[...])
        cos[n] = jnp.cos(angle)
        sin[n] = jnp.sin(angle) * jnp.where(freq_ref[...] < 0, -1, 1)
        return 0

    lax.fori_loop(0, owners, table, 0)
    actions(plan[0][first:])

    def step(i, _):
        c, j, slot = lax.rem(lax.div(i, nt), 2), lax.rem(i, nt), lax.rem(i, 2)
        for s in range(1, steps):
            if plan[s]:
                pl.when(i == s)(functools.partial(actions, plan[s]))

        @pl.when(i + 1 < steps)
        def _():
            weights(lax.rem(i + 1, nt), 1 - slot)

        @pl.when(j == 0)
        def _():
            pltpu.make_async_copy(xb.at[c], xb.at[c], xsem.at[c]).wait()

        weights_wait(j, slot)
        acc[...] = dot(xb.at[c].reshape(m_rows, dim)[...], wb[slot], 1, 0)

        @pl.when(i > 1)
        def _():
            results(i - 2, False)

        finish(i)
        results(i, True)
        return 0

    lax.fori_loop(0, steps, step, 0)
    actions(plan[-1])
    for i in (steps - 2, steps - 1):
        results(i, False)
    others = xg.at[pl.ds(0, owners - 1)]
    pltpu.make_async_copy(others, others, ssem).wait()


def gathered_qkv(x, gain, wq, wk, wv, owners):
    tokens, dim = x.shape
    heads = wq.shape[1] // HEAD
    freq = np.float32(THETA) ** (-np.arange(HALF, dtype=np.float32) / np.float32(HALF))
    freq = jnp.asarray(np.concatenate([-freq, freq])[None])
    lump = tokens // PIECES * LUMP
    plan = plan_gather((3 * heads + 1) // 2, 4.3)
    plan[TURN].append(("turn", None))
    out = jax.ShapeDtypeStruct((heads, owners, tokens, HEAD), LOW)
    work = 2 * owners * tokens * dim * 3 * heads * HEAD
    _, q, k, v = pl.pallas_call(
        functools.partial(gather_kernel, plan),
        out_shape=[jax.ShapeDtypeStruct((owners, tokens, dim), LOW), out, out, out],
        in_specs=[ANYWHERE, NEAR, NEAR, ANYWHERE, ANYWHERE, ANYWHERE],
        out_specs=[ANYWHERE] * 4,
        scratch_shapes=[pltpu.VMEM((2, owners, lump, dim), LOW)]
        + [pltpu.VMEM((2, dim, 2 * HEAD), LOW), pltpu.VMEM((2, 2, owners, lump, HEAD), LOW), pltpu.VMEM((owners * lump, 2 * HEAD), WIDE)]
        + [pltpu.VMEM((owners, tokens, HEAD), WIDE)] * 2
        + [DMA((PIECES,)), DMA((PIECES,)), DMA((2,)), DMA((2,)), DMA((2, 2)), DMA, DMA((PIECES, KINDS)), pltpu.SemaphoreType.REGULAR],
        compiler_params=pltpu.CompilerParams(collective_id=1, has_side_effects=True, vmem_limit_bytes=VMEM),
        cost_estimate=pl.CostEstimate(flops=work, transcendentals=0, bytes_accessed=dim * dim),
        name="gather_qkv",
    )(x, gain, freq, wq, wk, wv)
    whole = (heads, owners * tokens, HEAD)
    return q.reshape(whole), k.reshape(whole), v.reshape(whole)


BAND = 512
RING = 4
LATE = (0, 1, 3, 4, 5)


def scatter_kernel(seen, wo, x_ref, y_ref, a_s, w_s, t_s, s_s, h_in, f_in, h_out, f_out, hb_in, fb_in, hb_out, fb_out, x_s, y_s,
                   asem, wsem, xsem, ysem, h_r, f_r, h_t, f_t, hb_r, fb_r, hb_t, fb_t):
    heads, _, _, tokens, _ = seen.shape
    depth, dim = wo.shape
    half = BAND // 2
    bands = dim // 2 // BAND
    pos, at = place_in(lax.axis_index("tp"))
    kept = w_s.shape[1]

    def turned_by(path, d):
        return lax.rem(pos[path] + d + SIDE, SIDE)

    def columns(path, j):
        return pl.ds(pl.multiple_of(path * (dim // 2) + j * BAND, BAND), BAND)

    def near(path, last, way):
        d = 1 - 2 * way
        return at(path, d, 0) if last else at(path, 0, d)

    kinds = {"h": (h_out, h_in, h_t, h_r, False), "f": (f_out, f_in, f_t, f_r, False), "hb": (hb_out, hb_in, hb_t, hb_r, True), "fb": (fb_out, fb_in, fb_t, fb_r, True)}

    def links(kind, path, j):
        src, dst, sent, came, last = kinds[kind]
        o, i = lax.rem(j, src.shape[1]), lax.rem(j, dst.shape[1])
        return [
            pltpu.make_async_remote_copy(
                src.at[path, o, way], dst.at[path, i, way], sent.at[path, o, way], came.at[path, i, way], device_id={"tp": near(path, last, way)}, device_id_type=MESH
            )
            for way in BOTH
        ]

    def free(kind, path, j):
        @pl.when(j > 1)
        def _():
            for one in links(kind, path, j):
                one.wait_send()

    def arrived(kind, path, j):
        for one in links(kind, path, j):
            one.wait_recv()

    def post(kind, path, j):
        for one in links(kind, path, j):
            one.start()

    def term(path, n, d, j):
        b = turned_by(1 - path, d)
        rows = a_s[b] if path else a_s[:, b]
        t_s[path, n] = dot(rows.reshape(SIDE * tokens, depth), w_s[path, lax.rem(j, kept)], 1, 0).reshape(SIDE, tokens, BAND)

    def fetch_w(path, j):
        return pltpu.make_async_copy(wo.at[:, columns(path, j)], w_s.at[path, lax.rem(j, kept)], wsem.at[path, lax.rem(j, kept)])

    def fetch_x(path, j):
        return pltpu.make_async_copy(x_ref.at[:, columns(path, j)], x_s.at[path, lax.rem(j, 2)], xsem.at[path, lax.rem(j, 2)])

    def put_y(path, j):
        return pltpu.make_async_copy(y_s.at[path, lax.rem(j, 2)], y_ref.at[:, columns(path, j)], ysem.at[path, lax.rem(j, 2)])

    def part(way):
        return slice(way * half, (way + 1) * half)

    def each(f):
        lax.fori_loop(0, SIDE, lambda r, _: (f(r), 0)[1], 0)

    def slots(j):
        return lax.rem(j, 2), lax.rem(j, RING)

    def op1(path, j):
        free("h", path, j)
        o, _ = slots(j)

        def add(r):
            for way in BOTH:
                h_out[path, o, way, r] = t_s[path, 0, r, :, part(way)].astype(LOW)

        each(add)
        post("h", path, j)

    def op2(path, j):
        arrived("h", path, j)
        free("f", path, j)
        o, i = slots(j)

        def add(r):
            for way in BOTH:
                f_out[path, o, way, r, :, part(way)] = (t_s[path, 1 + way, r, :, part(way)] + h_in[path, i, way, r].astype(WIDE)).astype(LOW)
                f_out[path, o, way, r, :, part(1 - way)] = t_s[path, 1 + way, r, :, part(1 - way)].astype(LOW)

        each(add)
        post("f", path, j)

    def op3(path, j):
        arrived("f", path, j)
        free("hb", path, j)
        o, i = slots(j)

        def add(r):
            s_s[path, i, r] = t_s[path, 3, r] + f_in[path, i, 0, r].astype(WIDE) + f_in[path, i, 1, r].astype(WIDE)

        each(add)
        far = turned_by(path, 2)
        for way in BOTH:
            hb_out[path, o, way] = s_s[path, i, far, :, part(way)].astype(LOW)
        post("hb", path, j)

    def op4(path, j):
        arrived("hb", path, j)
        free("fb", path, j)
        o, i = slots(j)
        for way in BOTH:
            r = turned_by(path, 1 - 2 * way)
            fb_out[path, o, way, :, part(way)] = (s_s[path, i, r, :, part(way)] + hb_in[path, o, way].astype(WIDE)).astype(LOW)
            fb_out[path, o, way, :, part(1 - way)] = s_s[path, i, r, :, part(1 - way)].astype(LOW)
        post("fb", path, j)
        fetch_x(path, j).start()

    def op5(path, j):
        arrived("fb", path, j)
        fetch_x(path, j).wait()

        @pl.when(j > 1)
        def _():
            put_y(path, j).wait()

        o, i = slots(j)
        total = s_s[path, i, pos[path]] + fb_in[path, o, 0].astype(WIDE) + fb_in[path, o, 1].astype(WIDE)
        y_s[path, o] = (x_s[path, o].astype(WIDE) + total).astype(LOW)
        put_y(path, j).start()

    fetch_a = [pltpu.make_async_copy(seen.at[h], a_s.at[:, :, :, pl.ds(h * HEAD, HEAD)], asem.at[h]) for h in range(heads)]
    for one in fetch_a:
        one.start()
    for path in BOTH:
        fetch_w(path, 0).start()
    met = greet([{"tp": near(path, True, way)} for path in BOTH for way in BOTH])
    for one in fetch_a:
        one.wait()
    met()

    def step(i, _):
        @pl.when(i + 1 < bands)
        def _():
            for path in BOTH:
                fetch_w(path, i + 1).start()

        def run(n, f):
            j = i - LATE[n]

            @pl.when((j >= 0) & (j < bands))
            def _():
                f(j)

        def start(j):
            for path in BOTH:
                fetch_w(path, j).wait()
            for path in BOTH:
                term(path, 0, 2, j)
            for path in BOTH:
                op1(path, j)

        def terms(*which):
            def f(j):
                for path in BOTH:
                    for n, d in which:
                        term(path, n, d, j)

            return f

        run(0, start)
        run(1, terms((1, 1), (2, -1)))
        run(2, terms((3, 0)))
        for n, op in ((4, op5), (3, op4), (2, op3), (1, op2)):
            run(n, lambda j, op=op: [op(path, j) for path in BOTH])
        return 0

    lax.fori_loop(0, bands + LATE[-1], step, 0)
    for path in BOTH:
        for j in (bands - 2, bands - 1):
            for kind in kinds:
                for one in links(kind, path, j):
                    one.wait_send()
            put_y(path, j).wait()


def scattered(seen, wo, x):
    heads, rows, _ = seen.shape
    tokens, dim = x.shape
    depth = wo.shape[0]
    low = lambda *shape: pltpu.VMEM((2, *shape), LOW)
    wide = lambda *shape: pltpu.VMEM((2, *shape, SIDE, tokens, BAND), WIDE)
    widths = (BAND // 2, BAND)
    large = [low(n, 2, SIDE, tokens, w) for n in (RING, 2) for w in widths]
    small = [low(2, 2, tokens, w) for _ in BOTH for w in widths]
    sems = [DMA((2, n, 2)) for n in (RING, RING, 2, 2, 2, 2, 2, 2)]
    return pl.pallas_call(
        scatter_kernel,
        out_shape=jax.ShapeDtypeStruct((tokens, dim), LOW),
        in_specs=[ANYWHERE] * 3,
        out_specs=ANYWHERE,
        scratch_shapes=[pltpu.VMEM((SIDE, SIDE, tokens, depth), LOW), low(5, depth, BAND), wide(4), wide(RING)]
        + large
        + small
        + [low(2, tokens, BAND)] * 2
        + [DMA((heads,)), DMA((2, 5)), DMA((2, 2)), DMA((2, 2))]
        + sems,
        compiler_params=pltpu.CompilerParams(collective_id=2, has_side_effects=True, vmem_limit_bytes=VMEM),
        cost_estimate=pl.CostEstimate(flops=2 * rows * depth * dim, transcendentals=0, bytes_accessed=4 * depth * dim),
        name="scatter_sum",
    )(seen.reshape(heads, SIDE, SIDE, tokens, HEAD), wo, x)


def solution(mesh):
    owners = mesh.shape["tp"]

    def step(x, gain, wq, wk, wv, wo):
        q, k, v = gathered_qkv(x, gain, wq, wk, wv, owners)
        return scattered(attend(q, k, v), wo, x)

    tokens, columns = P(("dp", "tp"), None), P(None, "tp")
    return jax.shard_map(
        step,
        mesh=mesh,
        in_specs=(tokens, P(None), columns, columns, columns, P("tp", None)),
        out_specs=tokens,
        check_vma=False,
    )
```

```python
import functools
import heapq
import itertools

import jax
import jax.numpy as jnp
import numpy as np
from jax import lax
from jax.experimental import pallas as pl
from jax.experimental.pallas import tpu as pltpu
from jax.sharding import PartitionSpec as P

NEG = -1e30
HIDDEN = 2 * NEG
LOG2E = 1.4426950408889634
HEAD = 128
HALF = HEAD // 2
THETA = 10000
EPSILON = 1e-6
VMEM = 62 * 2**20
MESH = pl.DeviceIdType.MESH
ANYWHERE = pl.BlockSpec(memory_space=pl.ANY)
NEAR = pl.BlockSpec(memory_space=pltpu.VMEM)
LOW, WIDE = jnp.bfloat16, jnp.float32
DMA = pltpu.SemaphoreType.DMA
BOTH = (0, 1)


def fit(size, want):
    return max(n for n in range(HEAD, max(min(want, size), HEAD) + 1, HEAD) if size % n == 0)


def dot(a, b, ca, cb):
    return lax.dot_general(a, b, (((ca,), (cb,)), ((), ())), preferred_element_type=WIDE)


BLOCK = 512
CUTS = 4


def attention_kernel(q_ref, k_ref, v_ref, o_ref, top_s, mix_s, gap_s):
    heads, bq, d = q_ref.shape
    iq = pl.program_id(0)
    e = d**-0.5 * LOG2E
    gap_s[...] = lax.broadcasted_iota(jnp.int32, (bq, bq), 1) - lax.broadcasted_iota(jnp.int32, (bq, bq), 0)
    for h in range(heads):
        top_s[h : h + 1, :] = jnp.full((1, bq), NEG, WIDE)
        mix_s[h] = jnp.zeros(mix_s.shape[1:], WIDE)
    ones = jnp.ones((mix_s.shape[1] - d, bq), LOW)

    def block(at, size, lo, masked):
        here, qs = pl.ds(pl.multiple_of(at, HEAD), size), slice(lo, bq)
        scores = [dot(k_ref[h, here, :], q_ref[h, qs, :], 1, 1) for h in range(heads)]
        weights, keeps = [], []
        for h, s in enumerate(scores):
            if masked:
                s = jnp.where(gap_s[:size, : bq - lo] >= 0, s, HIDDEN)
            old = top_s[h : h + 1, qs]
            top = jnp.maximum(old, s.max(axis=0, keepdims=True))
            top_s[h : h + 1, qs] = top
            weights.append(jnp.exp2((s - top) * e).astype(LOW))
            keeps.append(jnp.exp2((old - top) * e))
        for h, (p, keep) in enumerate(zip(weights, keeps)):
            values = jnp.concatenate([v_ref[h, here, :].T, ones[:, :size]], axis=0)
            mix_s[h, :, qs] = mix_s[h, :, qs] * keep + dot(values, p, 1, 0)

    lax.fori_loop(0, iq, lambda j, _: block(j * bq, bq, 0, False), None)
    part = bq // CUTS
    for n in range(CUTS):
        block(iq * bq + n * part, part, n * part, True)
    for h in range(heads):
        o_ref[h] = (mix_s[h, :d, :] * (1 / mix_s[h, d : d + 1, :])).T.astype(o_ref.dtype)


def attend(q, k, v):
    heads, tokens, d = q.shape
    bq = fit(tokens, BLOCK)
    some = pl.BlockSpec((heads, bq, d), lambda i: (0, i, 0))
    return pl.pallas_call(
        attention_kernel,
        grid=(tokens // bq,),
        in_specs=[some, NEAR, NEAR],
        out_specs=some,
        out_shape=jax.ShapeDtypeStruct(q.shape, q.dtype),
        scratch_shapes=[pltpu.VMEM((heads, bq), WIDE), pltpu.VMEM((heads, d + 8, bq), WIDE), pltpu.VMEM((bq, bq), jnp.int32)],
        compiler_params=pltpu.CompilerParams(dimension_semantics=("arbitrary",), vmem_limit_bytes=VMEM),
        cost_estimate=pl.CostEstimate(flops=4 * q.size * tokens, transcendentals=heads * tokens**2, bytes_accessed=8 * q.size),
        name="attention",
    )(q, k, v)


SIDE = 4
PIECES = 4
LUMP = 1
TURN = 16
KINDS = 48


def plan_gather(tiles, tile_us):
    free, queue, done, groups, count = {}, [], [0] * PIECES, [[]], itertools.count()
    rate, delay = PIECES * 0.051, 8

    def send(t, m):
        stage, _, path, kind, sign, half = m
        link = (path if stage == 1 else 1 - path, sign)
        size = (1 if kind < 3 or stage == 1 else 0.5) * (0.5 if half else 1)
        free[link] = max(t, free.get(link, 0)) + size / rate
        heapq.heappush(queue, (free[link] + delay, next(count), m))
        groups[-1].append(("send", m))

    def begin(piece, t):
        for path in BOTH:
            for stage in (1, 2):
                for sign in (1, -1):
                    send(t, (stage, piece, path, 0, sign, 0))

    begun, t, tile, loaded = 1, 0, 0, 0
    begin(0, t)
    while queue or tile < tiles * PIECES // LUMP:
        while queue and queue[0][0] <= t:
            m = heapq.heappop(queue)[-1]
            groups[-1].append(("wait", m))
            stage, piece, path, kind, sign, half = m
            if stage == 1:
                if not half:
                    send(t, (1, piece, path, 0, sign, 1))
                kind = (1 if sign == 1 else 2) + 2 * half
                for way in (1, -1):
                    send(t, (2, piece, path, kind, way, 0))
            elif not half:
                send(t, (2, piece, path, kind, sign, 1))
            done[piece] += 1
            if begun < PIECES and done[begun - 1] * 3 >= KINDS:
                begin(begun, t)
                begun += 1
        while loaded * LUMP < PIECES and done[loaded * LUMP + LUMP - 1] == done[loaded * LUMP] == KINDS and tile >= (loaded - 1) * tiles:
            groups[-1].append(("load", loaded))
            loaded += 1
        if tile // tiles < loaded:
            groups.append([])
            tile += 1
            t += tile_us
        elif queue:
            t = max(t, queue[0][0])
    return groups


def place_in(t):
    pos = (lax.div(t, SIDE), lax.rem(t, SIDE))

    def at(path, da, db):
        a, b = lax.rem(pos[path] + da + SIDE, SIDE), lax.rem(pos[1 - path] + db + SIDE, SIDE)
        return a * SIDE + b if path == 0 else b * SIDE + a

    return pos, at


def greet(devices):
    barrier = pltpu.get_barrier_semaphore()
    for device in devices:
        pl.semaphore_signal(barrier, 1, device_id=device, device_id_type=MESH)
    return lambda: pl.semaphore_wait(barrier, len(devices))


def gather_kernel(plan, x_ref, gain_ref, freq_ref, wq, wk, wv, xg, q, k, v, xb, wb, ob, acc, cos, sin, bsem, lsem, xsem, wsem, osem, ssem, rsem, turn):
    owners, tokens, dim = xg.shape
    rows = tokens // PIECES
    lump = rows * LUMP
    m_rows = owners * lump
    split = dim // 2
    heads = q.shape[0]
    t = lax.axis_index("tp")
    pair = lax.axis_index("dp")
    second = lax.rem(pair, 2)
    other = {"dp": pair + 1 - 2 * second, "tp": t}
    _, at = place_in(t)

    def block(m, sending):
        stage, piece, path, kind, sign, half = m
        da, db, lo, width = 0, 0, 0, 4
        if stage == 1:
            da = -sign * half
            if half:
                width = 2
                lo = 1 - sign
        else:
            da, db = (0, -1, 1, 2, 2)[kind], -sign * half
            if kind > 2:
                width = 2
                lo = 2 * (kind - 3)
            if half:
                width //= 2
                lo += 0 if sign == 1 else width
        if not sending:
            da, db = (da - sign, db) if stage == 1 else (da, db - sign)
        return xg.at[at(path, da, db), pl.ds(piece * rows, rows), pl.ds(path * split + lo * split // 4, width * split // 4)]

    def message(m, sending):
        stage, piece, path, kind, sign, half = m
        key = (stage - 1) * 8 + path * 4 + kind * 8 + (sign + 1) // 2 + 2 * half
        here = block(m, sending)
        to = (at(path, sign, 0) if stage == 1 else at(path, 0, sign)) if sending else t
        return pltpu.make_async_remote_copy(here, here, ssem, rsem.at[piece, key], device_id={"tp": to}, device_id_type=MESH)

    given = ((wq, q), (wk, k), (wv, v))
    arrays = range(len(given))
    even = heads - heads % 2
    units = [(a, h) for a in arrays for h in range(even)] + [(a, h) for h in range(even, heads) for a in arrays]
    tiles = [units[n : n + 2] for n in range(0, len(units), 2)]
    nt = len(tiles)
    steps = nt * PIECES // LUMP

    pairs = even // 2
    whole = pairs * len(given)

    def among(i, n, f, first=0):
        if n - first == 1:
            f(first)
        elif n > first:
            mid = (first + n) // 2
            pl.when(i < mid)(lambda: among(i, mid, f, first))
            pl.when(i >= mid)(lambda: among(i, n, f, mid))

    def copies(j, f):
        @pl.when(j < whole)
        def _():
            among(lax.div(j, pairs), len(given), lambda a: f(a, pl.multiple_of(lax.rem(j, pairs) * 2, 2), 0, 2))

        if whole < nt:

            @pl.when(j >= whole)
            def _():
                among(j - whole, nt - whole, lambda n: [f(a, h, i, 1) for i, (a, h) in enumerate(tiles[whole + n])])

    def weights(j, slot):
        def go(a, h, i, n):
            src = given[a][0].at[:, pl.ds(pl.multiple_of(h * HEAD, HEAD), n * HEAD)]
            pltpu.make_async_copy(src, wb.at[slot, :, pl.ds(i * HEAD, n * HEAD)], wsem.at[slot]).start()

        copies(j, go)

    def sized(j, f):
        pl.when(j < nt - 1)(lambda: f(2))
        pl.when(j == nt - 1)(lambda: f(len(tiles[-1])))

    def weights_wait(j, slot):
        def go(n):
            part = wb.at[slot, :, pl.ds(0, n * HEAD)]
            pltpu.make_async_copy(part, part, wsem.at[slot]).wait()

        sized(j, go)

    def results(i):
        c, j, slot = lax.div(i, nt), lax.rem(i, nt), lax.rem(i, 2)
        here = pl.ds(pl.multiple_of(c * lump, lump), lump)

        def go(a, h, i, n):
            pltpu.make_async_copy(ob.at[slot, pl.ds(i, n)], given[a][1].at[pl.ds(h, n), :, here, :], osem.at[slot]).start()

        copies(j, go)

    def results_wait(i):
        def go(n):
            part = ob.at[lax.rem(i, 2), pl.ds(0, n)]
            pltpu.make_async_copy(part, part, osem.at[lax.rem(i, 2)]).wait()

        sized(lax.rem(i, nt), go)

    def finish(i):
        c, j, slot = lax.div(i, nt), lax.rem(i, nt), lax.rem(i, 2)
        here = pl.ds(pl.multiple_of(c * lump, lump), lump)
        turns = (j < 2 * pairs) | (j == whole) if nt > whole else j < 2 * pairs
        co, si = cos[:, here, :].reshape(m_rows, HEAD), sin[:, here, :].reshape(m_rows, HEAD)
        for n in BOTH:
            plain = acc[:, n * HEAD : (n + 1) * HEAD].astype(LOW).astype(WIDE)
            both = plain * co + pltpu.roll(plain, HALF, 1) * si
            ob[slot, n] = jnp.where(turns, both, plain).astype(LOW).reshape(owners, lump, HEAD)

    def load(c):
        return pltpu.make_async_copy(xg.at[:, pl.ds(c * lump, lump), :], xb.at[c % 2], xsem.at[c % 2])

    def actions(group):
        for what, m in group:
            if what == "send":
                message(m, True).start()
            elif what == "wait":
                message(m, False).wait_recv()
            elif what == "load":
                load(m).start()
            else:

                @pl.when(second == 0)
                def _():
                    pl.semaphore_signal(turn, 1, device_id=other, device_id_type=MESH)

    per = lump // rows

    def staged(n):
        return xb.at[1, n // per, pl.ds(n % per * rows, rows)]

    def raw(c):
        return pltpu.make_async_copy(x_ref.at[pl.ds(c * rows, rows), :], staged(c), lsem.at[c])

    def own(c):
        return pltpu.make_async_copy(staged(PIECES + c), xg.at[t, pl.ds(c * rows, rows), :], bsem.at[c])

    wide = fit(dim, 1024)

    def norm(c):
        raw(c).wait()
        src, dst = staged(c), staged(PIECES + c)

        def square(n, total):
            part = src[:, pl.ds(pl.multiple_of(n * wide, wide), wide)].astype(WIDE)
            return total + part * part

        total = lax.fori_loop(0, dim // wide, square, jnp.zeros((rows, wide), WIDE))
        scale = lax.rsqrt(jnp.sum(total, -1, keepdims=True) * (1 / dim) + EPSILON)

        def scaled(n, _):
            here = pl.ds(pl.multiple_of(n * wide, wide), wide)
            dst[:, here] = (src[:, here].astype(WIDE) * scale * gain_ref[here].astype(WIDE)[None]).astype(LOW)
            return 0

        lax.fori_loop(0, dim // wide, scaled, 0)
        own(c).start()

    for c in range(PIECES):
        raw(c).start()
    met = greet([{"tp": near} for near in (at(0, 1, 0), at(0, -1, 0), at(0, 0, 1), at(0, 0, -1))] + [other])
    weights(0, 0)
    norm(0)
    met()

    @pl.when(second == 1)
    def _():
        for c in range(1, PIECES):
            norm(c)
        pl.semaphore_wait(turn, 1)

    own(0).wait()
    first = [n for n, (what, _) in enumerate(plan[0]) if what == "wait"][0]
    actions(plan[0][:first])

    @pl.when(second == 0)
    def _():
        for c in range(1, PIECES):
            norm(c)

    for c in range(1, PIECES):
        own(c).wait()

    def table(n, _):
        place = (lax.broadcasted_iota(jnp.int32, (tokens, HEAD), 0) + n * tokens).astype(WIDE)
        angle = place * jnp.abs(freq_ref[...])
        cos[n] = jnp.cos(angle)
        sin[n] = jnp.sin(angle) * jnp.where(freq_ref[...] < 0, -1, 1)
        return 0

    lax.fori_loop(0, owners, table, 0)
    actions(plan[0][first:])

    def step(i, _):
        c, j, slot = lax.rem(lax.div(i, nt), 2), lax.rem(i, nt), lax.rem(i, 2)
        among(i, steps, lambda n: actions(plan[n] if n else []))

        @pl.when(i + 1 < steps)
        def _():
            weights(lax.rem(i + 1, nt), 1 - slot)

        @pl.when(j == 0)
        def _():
            pltpu.make_async_copy(xb.at[c], xb.at[c], xsem.at[c]).wait()

        weights_wait(j, slot)

        @pl.when(i > 2)
        def _():
            results_wait(i - 3)

        last = jnp.maximum(i - 1, 0)
        finish(last)
        acc[...] = dot(xb.at[c].reshape(m_rows, dim)[...], wb[slot], 1, 0)

        @pl.when(i > 0)
        def _():
            results(last)

        return 0

    acc[...] = jnp.zeros(acc.shape, acc.dtype)
    lax.fori_loop(0, steps, step, 0)
    actions(plan[-1])
    results_wait(steps - 3)
    finish(steps - 1)
    results(steps - 1)
    results_wait(steps - 2)
    results_wait(steps - 1)
    others = xg.at[pl.ds(0, owners - 1)]
    pltpu.make_async_copy(others, others, ssem).wait()


def gathered_qkv(x, gain, wq, wk, wv, owners):
    tokens, dim = x.shape
    heads = wq.shape[1] // HEAD
    freq = np.float32(THETA) ** (-np.arange(HALF, dtype=np.float32) / np.float32(HALF))
    freq = jnp.asarray(np.concatenate([-freq, freq])[None])
    lump = tokens // PIECES * LUMP
    plan = plan_gather((3 * heads + 1) // 2, 5)
    plan[TURN].append(("turn", None))
    out = jax.ShapeDtypeStruct((heads, owners, tokens, HEAD), LOW)
    work = 2 * owners * tokens * dim * 3 * heads * HEAD
    _, q, k, v = pl.pallas_call(
        functools.partial(gather_kernel, plan),
        out_shape=[jax.ShapeDtypeStruct((owners, tokens, dim), LOW), out, out, out],
        in_specs=[ANYWHERE, NEAR, NEAR, ANYWHERE, ANYWHERE, ANYWHERE],
        out_specs=[ANYWHERE] * 4,
        scratch_shapes=[pltpu.VMEM((2, owners, lump, dim), LOW)]
        + [pltpu.VMEM((2, dim, 2 * HEAD), LOW), pltpu.VMEM((2, 2, owners, lump, HEAD), LOW), pltpu.VMEM((owners * lump, 2 * HEAD), WIDE)]
        + [pltpu.VMEM((owners, tokens, HEAD), WIDE)] * 2
        + [DMA((PIECES,)), DMA((PIECES,)), DMA((2,)), DMA((2,)), DMA((2,)), DMA, DMA((PIECES, KINDS)), pltpu.SemaphoreType.REGULAR],
        compiler_params=pltpu.CompilerParams(collective_id=1, has_side_effects=True, vmem_limit_bytes=VMEM),
        cost_estimate=pl.CostEstimate(flops=work, transcendentals=0, bytes_accessed=dim * dim),
        name="gather_qkv",
    )(x, gain, freq, wq, wk, wv)
    whole = (heads, owners * tokens, HEAD)
    return q.reshape(whole), k.reshape(whole), v.reshape(whole)


BAND = 512
RING = 4
LATE = (0, 1, 3, 4, 5)


def scatter_kernel(seen, wo, x_ref, y_ref, a_s, w_s, t_s, s_s, h_in, f_in, h_out, f_out, hb_in, fb_in, hb_out, fb_out, x_s, y_s,
                   asem, wsem, xsem, ysem, h_r, f_r, h_t, f_t, hb_r, fb_r, hb_t, fb_t):
    heads, _, _, tokens, _ = seen.shape
    depth, dim = wo.shape
    half = BAND // 2
    bands = dim // 2 // BAND
    pos, at = place_in(lax.axis_index("tp"))
    kept = w_s.shape[1]

    def turned_by(path, d):
        return lax.rem(pos[path] + d + SIDE, SIDE)

    def columns(path, j):
        return pl.ds(pl.multiple_of(path * (dim // 2) + j * BAND, BAND), BAND)

    def near(path, last, way):
        d = 1 - 2 * way
        return at(path, d, 0) if last else at(path, 0, d)

    kinds = {"h": (h_out, h_in, h_t, h_r, False), "f": (f_out, f_in, f_t, f_r, False), "hb": (hb_out, hb_in, hb_t, hb_r, True), "fb": (fb_out, fb_in, fb_t, fb_r, True)}

    def links(kind, path, j):
        src, dst, sent, came, last = kinds[kind]
        o, i = lax.rem(j, src.shape[1]), lax.rem(j, dst.shape[1])
        return [
            pltpu.make_async_remote_copy(
                src.at[path, o, way], dst.at[path, i, way], sent.at[path, o, way], came.at[path, i, way], device_id={"tp": near(path, last, way)}, device_id_type=MESH
            )
            for way in BOTH
        ]

    def free(kind, path, j):
        @pl.when(j > 1)
        def _():
            for one in links(kind, path, j):
                one.wait_send()

    def arrived(kind, path, j):
        for one in links(kind, path, j):
            one.wait_recv()

    def post(kind, path, j):
        for one in links(kind, path, j):
            one.start()

    def term(path, n, d, j):
        b = turned_by(1 - path, d)
        rows = a_s[b] if path else a_s[:, b]
        t_s[path, n] = dot(rows.reshape(SIDE * tokens, depth), w_s[path, lax.rem(j, kept)], 1, 0).reshape(SIDE, tokens, BAND)

    def fetch_w(path, j):
        return pltpu.make_async_copy(wo.at[:, columns(path, j)], w_s.at[path, lax.rem(j, kept)], wsem.at[path, lax.rem(j, kept)])

    def fetch_x(path, j):
        return pltpu.make_async_copy(x_ref.at[:, columns(path, j)], x_s.at[path, lax.rem(j, 2)], xsem.at[path, lax.rem(j, 2)])

    def put_y(path, j):
        return pltpu.make_async_copy(y_s.at[path, lax.rem(j, 2)], y_ref.at[:, columns(path, j)], ysem.at[path, lax.rem(j, 2)])

    def part(way):
        return slice(way * half, (way + 1) * half)

    def each(f):
        lax.fori_loop(0, SIDE, lambda r, _: (f(r), 0)[1], 0)

    def slots(j):
        return lax.rem(j, 2), lax.rem(j, RING)

    def op1(path, j):
        free("h", path, j)
        o, _ = slots(j)

        def add(r):
            for way in BOTH:
                h_out[path, o, way, r] = t_s[path, 0, r, :, part(way)].astype(LOW)

        each(add)
        post("h", path, j)

    def op2(path, j):
        arrived("h", path, j)
        free("f", path, j)
        o, i = slots(j)

        def add(r):
            for way in BOTH:
                f_out[path, o, way, r, :, part(way)] = (t_s[path, 1 + way, r, :, part(way)] + h_in[path, i, way, r].astype(WIDE)).astype(LOW)
                f_out[path, o, way, r, :, part(1 - way)] = t_s[path, 1 + way, r, :, part(1 - way)].astype(LOW)

        each(add)
        post("f", path, j)

    def op3(path, j):
        arrived("f", path, j)
        free("hb", path, j)
        o, i = slots(j)

        def add(r):
            s_s[path, i, r] = t_s[path, 3, r] + f_in[path, i, 0, r].astype(WIDE) + f_in[path, i, 1, r].astype(WIDE)

        each(add)
        far = turned_by(path, 2)
        for way in BOTH:
            hb_out[path, o, way] = s_s[path, i, far, :, part(way)].astype(LOW)
        post("hb", path, j)

    def op4(path, j):
        arrived("hb", path, j)
        free("fb", path, j)
        o, i = slots(j)
        for way in BOTH:
            r = turned_by(path, 1 - 2 * way)
            fb_out[path, o, way, :, part(way)] = (s_s[path, i, r, :, part(way)] + hb_in[path, o, way].astype(WIDE)).astype(LOW)
            fb_out[path, o, way, :, part(1 - way)] = s_s[path, i, r, :, part(1 - way)].astype(LOW)
        post("fb", path, j)
        fetch_x(path, j).start()

    def op5(path, j):
        arrived("fb", path, j)
        fetch_x(path, j).wait()

        @pl.when(j > 1)
        def _():
            put_y(path, j).wait()

        o, i = slots(j)
        total = s_s[path, i, pos[path]] + fb_in[path, o, 0].astype(WIDE) + fb_in[path, o, 1].astype(WIDE)
        y_s[path, o] = (x_s[path, o].astype(WIDE) + total).astype(LOW)
        put_y(path, j).start()

    fetch_a = [pltpu.make_async_copy(seen.at[h], a_s.at[:, :, :, pl.ds(h * HEAD, HEAD)], asem.at[h]) for h in range(heads)]
    for one in fetch_a:
        one.start()
    for path in BOTH:
        fetch_w(path, 0).start()
    met = greet([{"tp": near(path, True, way)} for path in BOTH for way in BOTH])
    for one in fetch_a:
        one.wait()
    met()

    def step(i, _):
        @pl.when(i + 1 < bands)
        def _():
            for path in BOTH:
                fetch_w(path, i + 1).start()

        def run(n, f):
            j = i - LATE[n]

            @pl.when((j >= 0) & (j < bands))
            def _():
                f(j)

        def start(j):
            for path in BOTH:
                fetch_w(path, j).wait()
            for path in BOTH:
                term(path, 0, 2, j)
            for path in BOTH:
                op1(path, j)

        def terms(*which):
            def f(j):
                for path in BOTH:
                    for n, d in which:
                        term(path, n, d, j)

            return f

        run(0, start)
        run(1, terms((1, 1), (2, -1)))
        run(2, terms((3, 0)))
        for n, op in ((4, op5), (3, op4), (2, op3), (1, op2)):
            run(n, lambda j, op=op: [op(path, j) for path in BOTH])
        return 0

    lax.fori_loop(0, bands + LATE[-1], step, 0)
    for path in BOTH:
        for j in (bands - 2, bands - 1):
            for kind in kinds:
                for one in links(kind, path, j):
                    one.wait_send()
            put_y(path, j).wait()


def scattered(seen, wo, x):
    heads, rows, _ = seen.shape
    tokens, dim = x.shape
    depth = wo.shape[0]
    low = lambda *shape: pltpu.VMEM((2, *shape), LOW)
    wide = lambda *shape: pltpu.VMEM((2, *shape, SIDE, tokens, BAND), WIDE)
    widths = (BAND // 2, BAND)
    large = [low(n, 2, SIDE, tokens, w) for n in (RING, 2) for w in widths]
    small = [low(2, 2, tokens, w) for _ in BOTH for w in widths]
    sems = [DMA((2, n, 2)) for n in (RING, RING, 2, 2, 2, 2, 2, 2)]
    return pl.pallas_call(
        scatter_kernel,
        out_shape=jax.ShapeDtypeStruct((tokens, dim), LOW),
        in_specs=[ANYWHERE] * 3,
        out_specs=ANYWHERE,
        scratch_shapes=[pltpu.VMEM((SIDE, SIDE, tokens, depth), LOW), low(5, depth, BAND), wide(4), wide(RING)]
        + large
        + small
        + [low(2, tokens, BAND)] * 2
        + [DMA((heads,)), DMA((2, 5)), DMA((2, 2)), DMA((2, 2))]
        + sems,
        compiler_params=pltpu.CompilerParams(collective_id=2, has_side_effects=True, vmem_limit_bytes=VMEM),
        cost_estimate=pl.CostEstimate(flops=2 * rows * depth * dim, transcendentals=0, bytes_accessed=4 * depth * dim),
        name="scatter_sum",
    )(seen.reshape(heads, SIDE, SIDE, tokens, HEAD), wo, x)


def solution(mesh):
    owners = mesh.shape["tp"]

    def step(x, gain, wq, wk, wv, wo):
        q, k, v = gathered_qkv(x, gain, wq, wk, wv, owners)
        return scattered(attend(q, k, v), wo, x)

    tokens, columns = P(("dp", "tp"), None), P(None, "tp")
    return jax.shard_map(
        step,
        mesh=mesh,
        in_specs=(tokens, P(None), columns, columns, columns, P("tp", None)),
        out_specs=tokens,
        check_vma=False,
    )
```

```python
import functools
import heapq
import itertools

import jax
import jax.numpy as jnp
import numpy as np
from jax import lax
from jax.experimental import pallas as pl
from jax.experimental.pallas import tpu as pltpu
from jax.sharding import PartitionSpec as P

NEG = -1e30
HIDDEN = 2 * NEG
LOG2E = 1.4426950408889634
HEAD = 128
HALF = HEAD // 2
THETA = 10000
EPSILON = 1e-6
VMEM = 62 * 2**20
MESH = pl.DeviceIdType.MESH
ANYWHERE = pl.BlockSpec(memory_space=pl.ANY)
NEAR = pl.BlockSpec(memory_space=pltpu.VMEM)
LOW, WIDE = jnp.bfloat16, jnp.float32
DMA = pltpu.SemaphoreType.DMA
BOTH = (0, 1)


def fit(size, want):
    return max(n for n in range(HEAD, max(min(want, size), HEAD) + 1, HEAD) if size % n == 0)


def dot(a, b, ca, cb):
    return lax.dot_general(a, b, (((ca,), (cb,)), ((), ())), preferred_element_type=WIDE)


BLOCK = 512
CUTS = 4


def attention_kernel(q_ref, k_ref, v_ref, o_ref, top_s, mix_s, gap_s):
    heads, bq, d = q_ref.shape
    iq = pl.program_id(0)
    e = d**-0.5 * LOG2E
    gap_s[...] = lax.broadcasted_iota(jnp.int32, (bq, bq), 1) - lax.broadcasted_iota(jnp.int32, (bq, bq), 0)
    for h in range(heads):
        top_s[h : h + 1, :] = jnp.full((1, bq), NEG, WIDE)
        mix_s[h] = jnp.zeros(mix_s.shape[1:], WIDE)
    ones = jnp.ones((mix_s.shape[1] - d, bq), LOW)

    def block(at, size, lo, masked):
        here, qs = pl.ds(pl.multiple_of(at, HEAD), size), slice(lo, bq)
        scores = [dot(k_ref[h, here, :], q_ref[h, qs, :], 1, 1) for h in range(heads)]
        weights, keeps = [], []
        for h, s in enumerate(scores):
            if masked:
                s = jnp.where(gap_s[:size, : bq - lo] >= 0, s, HIDDEN)
            old = top_s[h : h + 1, qs]
            top = jnp.maximum(old, s.max(axis=0, keepdims=True))
            top_s[h : h + 1, qs] = top
            weights.append(jnp.exp2((s - top) * e).astype(LOW))
            keeps.append(jnp.exp2((old - top) * e))
        for h, (p, keep) in enumerate(zip(weights, keeps)):
            values = jnp.concatenate([v_ref[h, here, :].T, ones[:, :size]], axis=0)
            mix_s[h, :, qs] = mix_s[h, :, qs] * keep + dot(values, p, 1, 0)

    lax.fori_loop(0, iq, lambda j, _: block(j * bq, bq, 0, False), None)
    part = bq // CUTS
    for n in range(CUTS):
        block(iq * bq + n * part, part, n * part, True)
    for h in range(heads):
        o_ref[h] = (mix_s[h, :d, :] * (1 / mix_s[h, d : d + 1, :])).T.astype(o_ref.dtype)


def attend(q, k, v):
    heads, tokens, d = q.shape
    bq = fit(tokens, BLOCK)
    some = pl.BlockSpec((heads, bq, d), lambda i: (0, i, 0))
    return pl.pallas_call(
        attention_kernel,
        grid=(tokens // bq,),
        in_specs=[some, NEAR, NEAR],
        out_specs=some,
        out_shape=jax.ShapeDtypeStruct(q.shape, q.dtype),
        scratch_shapes=[pltpu.VMEM((heads, bq), WIDE), pltpu.VMEM((heads, d + 8, bq), WIDE), pltpu.VMEM((bq, bq), jnp.int32)],
        compiler_params=pltpu.CompilerParams(dimension_semantics=("arbitrary",), vmem_limit_bytes=VMEM),
        cost_estimate=pl.CostEstimate(flops=4 * q.size * tokens, transcendentals=heads * tokens**2, bytes_accessed=8 * q.size),
        name="attention",
    )(q, k, v)


SIDE = 4
PIECES = 8
LUMP = 2
TURN = 18
AHEAD = 2
KINDS = 48


def plan_gather(tiles, tile_us):
    free, queue, done, groups, count = {}, [], [0] * PIECES, [[]], itertools.count()
    rate, delay = PIECES * 0.06, 2.5

    def send(t, m):
        stage, _, path, kind, sign, half = m
        link = (path if stage == 1 else 1 - path, sign)
        size = (1 if kind < 3 or stage == 1 else 0.5) * (0.5 if half else 1)
        free[link] = max(t, free.get(link, 0)) + size / rate
        heapq.heappush(queue, (free[link] + delay, next(count), m))
        groups[-1].append(("send", m))

    def begin(piece, t):
        for path in BOTH:
            for stage in (1, 2):
                for sign in (1, -1):
                    send(t, (stage, piece, path, 0, sign, 0))

    begun, t, tile, loaded = AHEAD, 0, 0, 0
    for n in range(AHEAD):
        begin(n, t)
    while queue or tile < tiles * PIECES // LUMP:
        while queue and queue[0][0] <= t:
            m = heapq.heappop(queue)[-1]
            groups[-1].append(("wait", m))
            stage, piece, path, kind, sign, half = m
            if stage == 1:
                if not half:
                    send(t, (1, piece, path, 0, sign, 1))
                kind = (1 if sign == 1 else 2) + 2 * half
                for way in (1, -1):
                    send(t, (2, piece, path, kind, way, 0))
            elif not half:
                send(t, (2, piece, path, kind, sign, 1))
            done[piece] += 1
            if begun < PIECES and done[begun - AHEAD] * 5 >= KINDS * 4:
                begin(begun, t)
                begun += 1
        while loaded * LUMP < PIECES and done[loaded * LUMP + LUMP - 1] == done[loaded * LUMP] == KINDS and tile >= (loaded - 1) * tiles:
            groups[-1].append(("load", loaded))
            loaded += 1
        if tile // tiles < loaded:
            groups.append([])
            tile += 1
            t += tile_us
        elif queue:
            t = max(t, queue[0][0])
    return groups


def place_in(t):
    pos = (lax.div(t, SIDE), lax.rem(t, SIDE))

    def at(path, da, db):
        a, b = lax.rem(pos[path] + da + SIDE, SIDE), lax.rem(pos[1 - path] + db + SIDE, SIDE)
        return a * SIDE + b if path == 0 else b * SIDE + a

    return pos, at


def greet(devices):
    barrier = pltpu.get_barrier_semaphore()
    for device in devices:
        pl.semaphore_signal(barrier, 1, device_id=device, device_id_type=MESH)
    return lambda: pl.semaphore_wait(barrier, len(devices))


def gather_kernel(plan, x_ref, gain_ref, freq_ref, wq, wk, wv, xg, q, k, v, xb, wb, ob, acc, cos, sin, bsem, lsem, xsem, wsem, osem, ssem, rsem, turn):
    owners, tokens, dim = xg.shape
    rows = tokens // PIECES
    lump = rows * LUMP
    m_rows = owners * lump
    split = dim // 2
    heads = q.shape[0]
    t = lax.axis_index("tp")
    pair = lax.axis_index("dp")
    second = lax.rem(pair, 2)
    other = {"dp": pair + 1 - 2 * second, "tp": t}
    _, at = place_in(t)

    def block(m, sending):
        stage, piece, path, kind, sign, half = m
        da, db, lo, width = 0, 0, 0, 4
        if stage == 1:
            da = -sign * half
            if half:
                width = 2
                lo = 1 - sign
        else:
            da, db = (0, -1, 1, 2, 2)[kind], -sign * half
            if kind > 2:
                width = 2
                lo = 2 * (kind - 3)
            if half:
                width //= 2
                lo += 0 if sign == 1 else width
        if not sending:
            da, db = (da - sign, db) if stage == 1 else (da, db - sign)
        return xg.at[at(path, da, db), pl.ds(piece * rows, rows), pl.ds(path * split + lo * split // 4, width * split // 4)]

    def message(m, sending):
        stage, piece, path, kind, sign, half = m
        key = (stage - 1) * 8 + path * 4 + kind * 8 + (sign + 1) // 2 + 2 * half
        here = block(m, sending)
        to = (at(path, sign, 0) if stage == 1 else at(path, 0, sign)) if sending else t
        return pltpu.make_async_remote_copy(here, here, ssem, rsem.at[piece, key], device_id={"tp": to}, device_id_type=MESH)

    given = ((wq, q), (wk, k), (wv, v))
    arrays = range(len(given))
    even = heads - heads % 2
    units = [(a, h) for a in arrays for h in range(even)] + [(a, h) for h in range(even, heads) for a in arrays]
    tiles = [units[n : n + 2] for n in range(0, len(units), 2)]
    nt = len(tiles)
    steps = nt * PIECES // LUMP

    pairs = even // 2
    whole = pairs * len(given)

    def among(i, n, f, first=0):
        if n - first == 1:
            f(first)
        elif n > first:
            mid = (first + n) // 2
            pl.when(i < mid)(lambda: among(i, mid, f, first))
            pl.when(i >= mid)(lambda: among(i, n, f, mid))

    def copies(j, f):
        @pl.when(j < whole)
        def _():
            among(lax.div(j, pairs), len(given), lambda a: f(a, pl.multiple_of(lax.rem(j, pairs) * 2, 2), 0, 2))

        if whole < nt:

            @pl.when(j >= whole)
            def _():
                among(j - whole, nt - whole, lambda n: [f(a, h, i, 1) for i, (a, h) in enumerate(tiles[whole + n])])

    def weights(j, slot):
        def go(a, h, i, n):
            src = given[a][0].at[:, pl.ds(pl.multiple_of(h * HEAD, HEAD), n * HEAD)]
            pltpu.make_async_copy(src, wb.at[slot, :, pl.ds(i * HEAD, n * HEAD)], wsem.at[slot]).start()

        copies(j, go)

    def sized(j, f):
        pl.when(j < nt - 1)(lambda: f(2))
        pl.when(j == nt - 1)(lambda: f(len(tiles[-1])))

    def weights_wait(j, slot):
        def go(n):
            part = wb.at[slot, :, pl.ds(0, n * HEAD)]
            pltpu.make_async_copy(part, part, wsem.at[slot]).wait()

        sized(j, go)

    def results(i):
        c, j, slot = lax.div(i, nt), lax.rem(i, nt), lax.rem(i, 2)
        here = pl.ds(pl.multiple_of(c * lump, lump), lump)

        def go(a, h, i, n):
            pltpu.make_async_copy(ob.at[slot, pl.ds(i, n)], given[a][1].at[pl.ds(h, n), :, here, :], osem.at[slot]).start()

        copies(j, go)

    def results_wait(i):
        def go(n):
            part = ob.at[lax.rem(i, 2), pl.ds(0, n)]
            pltpu.make_async_copy(part, part, osem.at[lax.rem(i, 2)]).wait()

        sized(lax.rem(i, nt), go)

    def finish(i):
        c, j, slot = lax.div(i, nt), lax.rem(i, nt), lax.rem(i, 2)
        here = pl.ds(pl.multiple_of(c * lump, lump), lump)
        turns = (j < 2 * pairs) | (j == whole) if nt > whole else j < 2 * pairs
        co, si = cos[:, here, :].reshape(m_rows, HEAD), sin[:, here, :].reshape(m_rows, HEAD)
        for n in BOTH:
            plain = acc[:, n * HEAD : (n + 1) * HEAD].astype(LOW).astype(WIDE)
            both = plain * co + pltpu.roll(plain, HALF, 1) * si
            ob[slot, n] = jnp.where(turns, both, plain).astype(LOW).reshape(owners, lump, HEAD)

    def load(c):
        return pltpu.make_async_copy(xg.at[:, pl.ds(c * lump, lump), :], xb.at[c % 2], xsem.at[c % 2])

    def actions(group):
        for what, m in group:
            if what == "send":
                message(m, True).start()
            elif what == "wait":
                message(m, False).wait_recv()
            elif what == "load":
                load(m).start()
            else:

                @pl.when(second == 0)
                def _():
                    pl.semaphore_signal(turn, 1, device_id=other, device_id_type=MESH)

    per = lump // rows

    def staged(n):
        return xb.at[1, n // per, pl.ds(n % per * rows, rows)]

    def raw(c):
        return pltpu.make_async_copy(x_ref.at[pl.ds(c * rows, rows), :], staged(c), lsem.at[c])

    def own(c):
        return pltpu.make_async_copy(staged(PIECES + c), xg.at[t, pl.ds(c * rows, rows), :], bsem.at[c])

    wide = fit(dim, 1024)

    def norm(c):
        raw(c).wait()
        src, dst = staged(c), staged(PIECES + c)

        def square(n, total):
            part = src[:, pl.ds(pl.multiple_of(n * wide, wide), wide)].astype(WIDE)
            return total + part * part

        total = lax.fori_loop(0, dim // wide, square, jnp.zeros((rows, wide), WIDE))
        scale = lax.rsqrt(jnp.sum(total, -1, keepdims=True) * (1 / dim) + EPSILON)

        def scaled(n, _):
            here = pl.ds(pl.multiple_of(n * wide, wide), wide)
            dst[:, here] = (src[:, here].astype(WIDE) * scale * gain_ref[here].astype(WIDE)[None]).astype(LOW)
            return 0

        lax.fori_loop(0, dim // wide, scaled, 0)
        own(c).start()

    for c in range(PIECES):
        raw(c).start()
    met = greet([{"tp": near} for near in (at(0, 1, 0), at(0, -1, 0), at(0, 0, 1), at(0, 0, -1))] + [other])
    weights(0, 0)
    for c in range(AHEAD):
        norm(c)
    met()

    @pl.when(second == 1)
    def _():
        for c in range(AHEAD, PIECES):
            norm(c)
        pl.semaphore_wait(turn, 1)

    for c in range(AHEAD):
        own(c).wait()
    first = [n for n, (what, _) in enumerate(plan[0]) if what == "wait"][0]
    actions(plan[0][:first])

    @pl.when(second == 0)
    def _():
        for c in range(AHEAD, PIECES):
            norm(c)

    for c in range(AHEAD, PIECES):
        own(c).wait()

    def table(n, _):
        place = (lax.broadcasted_iota(jnp.int32, (tokens, HEAD), 0) + n * tokens).astype(WIDE)
        angle = place * jnp.abs(freq_ref[...])
        cos[n] = jnp.cos(angle)
        sin[n] = jnp.sin(angle) * jnp.where(freq_ref[...] < 0, -1, 1)
        return 0

    lax.fori_loop(0, owners, table, 0)
    actions(plan[0][first:])

    def step(i, _):
        c, j, slot = lax.rem(lax.div(i, nt), 2), lax.rem(i, nt), lax.rem(i, 2)
        among(i, steps, lambda n: actions(plan[n] if n else []))

        @pl.when(i + 1 < steps)
        def _():
            weights(lax.rem(i + 1, nt), 1 - slot)

        @pl.when(j == 0)
        def _():
            pltpu.make_async_copy(xb.at[c], xb.at[c], xsem.at[c]).wait()

        weights_wait(j, slot)

        @pl.when(i > 2)
        def _():
            results_wait(i - 3)

        last = jnp.maximum(i - 1, 0)
        finish(last)
        acc[...] = dot(xb.at[c].reshape(m_rows, dim)[...], wb[slot], 1, 0)

        @pl.when(i > 0)
        def _():
            results(last)

        return 0

    acc[...] = jnp.zeros(acc.shape, acc.dtype)
    lax.fori_loop(0, steps, step, 0)
    actions(plan[-1])
    results_wait(steps - 3)
    finish(steps - 1)
    results(steps - 1)
    results_wait(steps - 2)
    results_wait(steps - 1)
    others = xg.at[pl.ds(0, owners - 1)]
    pltpu.make_async_copy(others, others, ssem).wait()


def gathered_qkv(x, gain, wq, wk, wv, owners):
    tokens, dim = x.shape
    heads = wq.shape[1] // HEAD
    freq = np.float32(THETA) ** (-np.arange(HALF, dtype=np.float32) / np.float32(HALF))
    freq = jnp.asarray(np.concatenate([-freq, freq])[None])
    lump = tokens // PIECES * LUMP
    plan = plan_gather((3 * heads + 1) // 2, 4.25)
    plan[TURN].append(("turn", None))
    out = jax.ShapeDtypeStruct((heads, owners, tokens, HEAD), LOW)
    work = 2 * owners * tokens * dim * 3 * heads * HEAD
    _, q, k, v = pl.pallas_call(
        functools.partial(gather_kernel, plan),
        out_shape=[jax.ShapeDtypeStruct((owners, tokens, dim), LOW), out, out, out],
        in_specs=[ANYWHERE, NEAR, NEAR, ANYWHERE, ANYWHERE, ANYWHERE],
        out_specs=[ANYWHERE] * 4,
        scratch_shapes=[pltpu.VMEM((2, owners, lump, dim), LOW)]
        + [pltpu.VMEM((2, dim, 2 * HEAD), LOW), pltpu.VMEM((2, 2, owners, lump, HEAD), LOW), pltpu.VMEM((owners * lump, 2 * HEAD), WIDE)]
        + [pltpu.VMEM((owners, tokens, HEAD), WIDE)] * 2
        + [DMA((PIECES,)), DMA((PIECES,)), DMA((2,)), DMA((2,)), DMA((2,)), DMA, DMA((PIECES, KINDS)), pltpu.SemaphoreType.REGULAR],
        compiler_params=pltpu.CompilerParams(collective_id=1, has_side_effects=True, vmem_limit_bytes=VMEM),
        cost_estimate=pl.CostEstimate(flops=work, transcendentals=0, bytes_accessed=dim * dim),
        name="gather_qkv",
    )(x, gain, freq, wq, wk, wv)
    whole = (heads, owners * tokens, HEAD)
    return q.reshape(whole), k.reshape(whole), v.reshape(whole)


BAND = 512
RING = 4
SUMS = 5
LATE = (0, 1, 3, 5, 7)


def scatter_kernel(seen, wo, x_ref, y_ref, a_s, w_s, t_s, s_s, h_in, f_in, h_out, f_out, hb_in, fb_in, hb_out, fb_out, x_s, y_s,
                   asem, wsem, xsem, ysem, h_r, f_r, h_t, f_t, hb_r, fb_r, hb_t, fb_t):
    heads, _, _, tokens, _ = seen.shape
    depth, dim = wo.shape
    half = BAND // 2
    bands = dim // 2 // BAND
    pos, at = place_in(lax.axis_index("tp"))
    kept = w_s.shape[1]

    def turned_by(path, d):
        return lax.rem(pos[path] + d + SIDE, SIDE)

    def columns(path, j):
        return pl.ds(pl.multiple_of(path * (dim // 2) + j * BAND, BAND), BAND)

    def near(path, last, way):
        d = 1 - 2 * way
        return at(path, d, 0) if last else at(path, 0, d)

    kinds = {"h": (h_out, h_in, h_t, h_r, False), "f": (f_out, f_in, f_t, f_r, False), "hb": (hb_out, hb_in, hb_t, hb_r, True), "fb": (fb_out, fb_in, fb_t, fb_r, True)}

    def links(kind, path, j):
        src, dst, sent, came, last = kinds[kind]
        o, i = lax.rem(j, src.shape[1]), lax.rem(j, dst.shape[1])
        return [
            pltpu.make_async_remote_copy(
                src.at[path, o, way], dst.at[path, i, way], sent.at[path, o, way], came.at[path, i, way], device_id={"tp": near(path, last, way)}, device_id_type=MESH
            )
            for way in BOTH
        ]

    def free(kind, path, j):
        @pl.when(j > 1)
        def _():
            for one in links(kind, path, j):
                one.wait_send()

    def arrived(kind, path, j):
        for one in links(kind, path, j):
            one.wait_recv()

    def post(kind, path, j):
        for one in links(kind, path, j):
            one.start()

    def term(path, n, d, j):
        b = turned_by(1 - path, d)
        rows = a_s[b] if path else a_s[:, b]
        t_s[path, n] = dot(rows.reshape(SIDE * tokens, depth), w_s[path, lax.rem(j, kept)], 1, 0).reshape(SIDE, tokens, BAND)

    def fetch_w(path, j):
        return pltpu.make_async_copy(wo.at[:, columns(path, j)], w_s.at[path, lax.rem(j, kept)], wsem.at[path, lax.rem(j, kept)])

    def fetch_x(path, j):
        return pltpu.make_async_copy(x_ref.at[:, columns(path, j)], x_s.at[path, lax.rem(j, 2)], xsem.at[path, lax.rem(j, 2)])

    def put_y(path, j):
        return pltpu.make_async_copy(y_s.at[path, lax.rem(j, 2)], y_ref.at[:, columns(path, j)], ysem.at[path, lax.rem(j, 2)])

    def part(way):
        return slice(way * half, (way + 1) * half)

    def each(f):
        lax.fori_loop(0, SIDE, lambda r, _: (f(r), 0)[1], 0)

    def slots(j):
        return lax.rem(j, 2), lax.rem(j, RING), lax.rem(j, SUMS)

    def op1(path, j):
        free("h", path, j)
        o, _, _ = slots(j)

        def add(r):
            for way in BOTH:
                h_out[path, o, way, r] = t_s[path, 0, r, :, part(way)].astype(LOW)

        each(add)
        post("h", path, j)

    def op2(path, j):
        arrived("h", path, j)
        free("f", path, j)
        o, i, _ = slots(j)

        def add(r):
            for way in BOTH:
                f_out[path, o, way, r, :, part(way)] = (t_s[path, 1 + way, r, :, part(way)] + h_in[path, i, way, r].astype(WIDE)).astype(LOW)
                f_out[path, o, way, r, :, part(1 - way)] = t_s[path, 1 + way, r, :, part(1 - way)].astype(LOW)

        each(add)
        post("f", path, j)

    def op3(path, j):
        arrived("f", path, j)
        free("hb", path, j)
        o, i, s = slots(j)

        def add(r):
            s_s[path, s, r] = t_s[path, 3, r] + f_in[path, i, 0, r].astype(WIDE) + f_in[path, i, 1, r].astype(WIDE)

        each(add)
        far = turned_by(path, 2)
        for way in BOTH:
            hb_out[path, o, way] = s_s[path, s, far, :, part(way)].astype(LOW)
        post("hb", path, j)

    def op4(path, j):
        arrived("hb", path, j)
        free("fb", path, j)
        o, i, s = slots(j)
        for way in BOTH:
            r = turned_by(path, 1 - 2 * way)
            fb_out[path, o, way, :, part(way)] = (s_s[path, s, r, :, part(way)] + hb_in[path, i, way].astype(WIDE)).astype(LOW)
            fb_out[path, o, way, :, part(1 - way)] = s_s[path, s, r, :, part(1 - way)].astype(LOW)
        post("fb", path, j)
        fetch_x(path, j).start()

    def op5(path, j):
        arrived("fb", path, j)
        fetch_x(path, j).wait()

        @pl.when(j > 1)
        def _():
            put_y(path, j).wait()

        o, i, s = slots(j)
        total = s_s[path, s, pos[path]] + fb_in[path, i, 0].astype(WIDE) + fb_in[path, i, 1].astype(WIDE)
        y_s[path, o] = (x_s[path, o].astype(WIDE) + total).astype(LOW)
        put_y(path, j).start()

    fetch_a = [pltpu.make_async_copy(seen.at[h], a_s.at[:, :, :, pl.ds(h * HEAD, HEAD)], asem.at[h]) for h in range(heads)]
    for one in fetch_a:
        one.start()
    for path in BOTH:
        fetch_w(path, 0).start()
    met = greet([{"tp": near(path, True, way)} for path in BOTH for way in BOTH])
    for one in fetch_a:
        one.wait()
    met()

    def step(i, _):
        @pl.when(i + 1 < bands)
        def _():
            for path in BOTH:
                fetch_w(path, i + 1).start()

        def run(n, f):
            j = i - LATE[n]

            @pl.when((j >= 0) & (j < bands))
            def _():
                f(j)

        def start(j):
            for path in BOTH:
                fetch_w(path, j).wait()
            for path in BOTH:
                term(path, 0, 2, j)
            for path in BOTH:
                op1(path, j)

        def terms(*which):
            def f(j):
                for path in BOTH:
                    for n, d in which:
                        term(path, n, d, j)

            return f

        run(0, start)
        run(1, terms((1, 1), (2, -1)))
        run(2, terms((3, 0)))
        for n, op in ((4, op5), (3, op4), (2, op3), (1, op2)):
            run(n, lambda j, op=op: [op(path, j) for path in BOTH])
        return 0

    lax.fori_loop(0, bands + LATE[-1], step, 0)
    for path in BOTH:
        for j in (bands - 2, bands - 1):
            for kind in kinds:
                for one in links(kind, path, j):
                    one.wait_send()
            put_y(path, j).wait()


def scattered(seen, wo, x):
    heads, rows, _ = seen.shape
    tokens, dim = x.shape
    depth = wo.shape[0]
    low = lambda *shape: pltpu.VMEM((2, *shape), LOW)
    wide = lambda *shape: pltpu.VMEM((2, *shape, SIDE, tokens, BAND), WIDE)
    widths = (BAND // 2, BAND)
    large = [low(n, 2, SIDE, tokens, w) for n in (RING, 2) for w in widths]
    small = [low(n, 2, tokens, w) for n in (RING, 2) for w in widths]
    sems = [DMA((2, n, 2)) for _ in BOTH for n in (RING, RING, 2, 2)]
    return pl.pallas_call(
        scatter_kernel,
        out_shape=jax.ShapeDtypeStruct((tokens, dim), LOW),
        in_specs=[ANYWHERE] * 3,
        out_specs=ANYWHERE,
        scratch_shapes=[pltpu.VMEM((SIDE, SIDE, tokens, depth), LOW), low(5, depth, BAND), wide(4), wide(SUMS)]
        + large
        + small
        + [low(2, tokens, BAND)] * 2
        + [DMA((heads,)), DMA((2, 5)), DMA((2, 2)), DMA((2, 2))]
        + sems,
        compiler_params=pltpu.CompilerParams(collective_id=2, has_side_effects=True, vmem_limit_bytes=VMEM),
        cost_estimate=pl.CostEstimate(flops=2 * rows * depth * dim, transcendentals=0, bytes_accessed=4 * depth * dim),
        name="scatter_sum",
    )(seen.reshape(heads, SIDE, SIDE, tokens, HEAD), wo, x)


def solution(mesh):
    owners = mesh.shape["tp"]

    def step(x, gain, wq, wk, wv, wo):
        q, k, v = gathered_qkv(x, gain, wq, wk, wv, owners)
        return scattered(attend(q, k, v), wo, x)

    tokens, columns = P(("dp", "tp"), None), P(None, "tp")
    return jax.shard_map(
        step,
        mesh=mesh,
        in_specs=(tokens, P(None), columns, columns, columns, P("tp", None)),
        out_specs=tokens,
        check_vma=False,
    )
```

```python
import functools
import heapq
import itertools

import jax
import jax.numpy as jnp
import numpy as np
from jax import lax
from jax.experimental import pallas as pl
from jax.experimental.pallas import tpu as pltpu
from jax.sharding import PartitionSpec as P

NEG = -1e30
HIDDEN = 2 * NEG
LOG2E = 1.4426950408889634
HEAD = 128
HALF = HEAD // 2
THETA = 10000
EPSILON = 1e-6
VMEM = 62 * 2**20
MESH = pl.DeviceIdType.MESH
ANYWHERE = pl.BlockSpec(memory_space=pl.ANY)
NEAR = pl.BlockSpec(memory_space=pltpu.VMEM)
LOW, WIDE = jnp.bfloat16, jnp.float32
DMA = pltpu.SemaphoreType.DMA
BOTH = (0, 1)


def fit(size, want):
    return max(n for n in range(HEAD, max(min(want, size), HEAD) + 1, HEAD) if size % n == 0)


def dot(a, b, ca, cb):
    return lax.dot_general(a, b, (((ca,), (cb,)), ((), ())), preferred_element_type=WIDE)


BLOCK = 512
CUTS = 4


def attention_kernel(q_ref, k_ref, v_ref, o_ref, top_s, mix_s, gap_s):
    heads, bq, d = q_ref.shape
    iq = pl.program_id(0)
    e = d**-0.5 * LOG2E
    gap_s[...] = lax.broadcasted_iota(jnp.int32, (bq, bq), 1) - lax.broadcasted_iota(jnp.int32, (bq, bq), 0)
    for h in range(heads):
        top_s[h : h + 1, :] = jnp.full((1, bq), NEG, WIDE)
        mix_s[h] = jnp.zeros(mix_s.shape[1:], WIDE)
    ones = jnp.ones((mix_s.shape[1] - d, 2 * bq), LOW)

    def block(at, size, lo, masked):
        here, qs = pl.ds(pl.multiple_of(at, HEAD), size), slice(lo, bq)
        scores = [dot(k_ref[h, here, :], q_ref[h, qs, :], 1, 1) for h in range(heads)]
        weights, keeps = [], []
        for h, s in enumerate(scores):
            if masked:
                s = jnp.where(gap_s[:size, : bq - lo] >= 0, s, HIDDEN)
            old = top_s[h : h + 1, qs]
            top = jnp.maximum(old, s.max(axis=0, keepdims=True))
            top_s[h : h + 1, qs] = top
            weights.append(jnp.exp2((s - top) * e).astype(LOW))
            keeps.append(jnp.exp2((old - top) * e))
        for h, (p, keep) in enumerate(zip(weights, keeps)):
            values = jnp.concatenate([v_ref[h, here, :].T, ones[:, :size]], axis=0)
            mix_s[h, :, qs] = mix_s[h, :, qs] * keep + dot(values, p, 1, 0)

    lax.fori_loop(0, lax.div(iq, 2), lambda j, _: block(2 * j * bq, 2 * bq, 0, False), None)
    pl.when(lax.rem(iq, 2) == 1)(lambda: block((iq - 1) * bq, bq, 0, False))
    part = bq // CUTS
    for n in range(CUTS):
        block(iq * bq + n * part, part, n * part, True)
    for h in range(heads):
        o_ref[h] = (mix_s[h, :d, :] * (1 / mix_s[h, d : d + 1, :])).T.astype(o_ref.dtype)


def attend(q, k, v):
    heads, tokens, d = q.shape
    bq = fit(tokens, BLOCK)
    some = pl.BlockSpec((heads, bq, d), lambda i: (0, i, 0))
    return pl.pallas_call(
        attention_kernel,
        grid=(tokens // bq,),
        in_specs=[some, NEAR, NEAR],
        out_specs=some,
        out_shape=jax.ShapeDtypeStruct(q.shape, q.dtype),
        scratch_shapes=[pltpu.VMEM((heads, bq), WIDE), pltpu.VMEM((heads, d + 8, bq), WIDE), pltpu.VMEM((bq, bq), jnp.int32)],
        compiler_params=pltpu.CompilerParams(dimension_semantics=("arbitrary",), vmem_limit_bytes=VMEM),
        cost_estimate=pl.CostEstimate(flops=4 * q.size * tokens, transcendentals=heads * tokens**2, bytes_accessed=8 * q.size),
        name="attention",
    )(q, k, v)


SIDE = 4
PIECES = 8
LUMP = 2
TURN = 19
AHEAD = 2
KINDS = 48


def plan_gather(tiles, tile_us):
    free, queue, done, groups, count = {}, [], [0] * PIECES, [[]], itertools.count()
    rate, delay = PIECES * 0.06, 2.5

    def send(t, m):
        stage, _, path, kind, sign, half = m
        link = (path if stage == 1 else 1 - path, sign)
        size = (1 if kind < 3 or stage == 1 else 0.5) * (0.5 if half else 1)
        free[link] = max(t, free.get(link, 0)) + size / rate
        heapq.heappush(queue, (free[link] + delay, next(count), m))
        groups[-1].append(("send", m))

    def begin(piece, t):
        for path in BOTH:
            for stage in (1, 2):
                for sign in (1, -1):
                    send(t, (stage, piece, path, 0, sign, 0))

    begun, t, tile, loaded = AHEAD, 0, 0, 0
    for n in range(AHEAD):
        begin(n, t)
    while queue or tile < tiles * PIECES // LUMP:
        while queue and queue[0][0] <= t:
            m = heapq.heappop(queue)[-1]
            groups[-1].append(("wait", m))
            stage, piece, path, kind, sign, half = m
            if stage == 1:
                if not half:
                    send(t, (1, piece, path, 0, sign, 1))
                kind = (1 if sign == 1 else 2) + 2 * half
                for way in (1, -1):
                    send(t, (2, piece, path, kind, way, 0))
            elif not half:
                send(t, (2, piece, path, kind, sign, 1))
            done[piece] += 1
            if begun < PIECES and done[begun - AHEAD] * 5 >= KINDS * 4:
                begin(begun, t)
                begun += 1
        while loaded * LUMP < PIECES and done[loaded * LUMP + LUMP - 1] == done[loaded * LUMP] == KINDS and tile >= (loaded - 1) * tiles:
            groups[-1].append(("load", loaded))
            loaded += 1
        if tile // tiles < loaded:
            groups.append([])
            tile += 1
            t += tile_us
        elif queue:
            t = max(t, queue[0][0])
    return groups


def place_in(t):
    pos = (lax.div(t, SIDE), lax.rem(t, SIDE))

    def at(path, da, db):
        a, b = lax.rem(pos[path] + da + SIDE, SIDE), lax.rem(pos[1 - path] + db + SIDE, SIDE)
        return a * SIDE + b if path == 0 else b * SIDE + a

    return pos, at


def greet(devices):
    barrier = pltpu.get_barrier_semaphore()
    for device in devices:
        pl.semaphore_signal(barrier, 1, device_id=device, device_id_type=MESH)
    return lambda: pl.semaphore_wait(barrier, len(devices))


def gather_kernel(plan, x_ref, gain_ref, freq_ref, wq, wk, wv, xg, q, k, v, xb, wb, ob, acc, cos, sin, bsem, lsem, xsem, wsem, osem, ssem, rsem, turn):
    owners, tokens, dim = xg.shape
    rows = tokens // PIECES
    lump = rows * LUMP
    m_rows = owners * lump
    split = dim // 2
    heads = q.shape[0]
    t = lax.axis_index("tp")
    pair = lax.axis_index("dp")
    second = lax.rem(pair, 2)
    other = {"dp": pair + 1 - 2 * second, "tp": t}
    _, at = place_in(t)

    def block(m, sending):
        stage, piece, path, kind, sign, half = m
        da, db, lo, width = 0, 0, 0, 4
        if stage == 1:
            da = -sign * half
            if half:
                width = 2
                lo = 1 - sign
        else:
            da, db = (0, -1, 1, 2, 2)[kind], -sign * half
            if kind > 2:
                width = 2
                lo = 2 * (kind - 3)
            if half:
                width //= 2
                lo += 0 if sign == 1 else width
        if not sending:
            da, db = (da - sign, db) if stage == 1 else (da, db - sign)
        return xg.at[at(path, da, db), pl.ds(piece * rows, rows), pl.ds(path * split + lo * split // 4, width * split // 4)]

    def message(m, sending):
        stage, piece, path, kind, sign, half = m
        key = (stage - 1) * 8 + path * 4 + kind * 8 + (sign + 1) // 2 + 2 * half
        here = block(m, sending)
        to = (at(path, sign, 0) if stage == 1 else at(path, 0, sign)) if sending else t
        return pltpu.make_async_remote_copy(here, here, ssem, rsem.at[piece, key], device_id={"tp": to}, device_id_type=MESH)

    given = ((wq, q), (wk, k), (wv, v))
    arrays = range(len(given))
    even = heads - heads % 2
    units = [(a, h) for a in arrays for h in range(even)] + [(a, h) for h in range(even, heads) for a in arrays]
    tiles = [units[n : n + 2] for n in range(0, len(units), 2)]
    nt = len(tiles)
    steps = nt * PIECES // LUMP

    pairs = even // 2
    whole = pairs * len(given)

    def among(i, n, f, first=0):
        if n - first == 1:
            f(first)
        elif n > first:
            mid = (first + n) // 2
            pl.when(i < mid)(lambda: among(i, mid, f, first))
            pl.when(i >= mid)(lambda: among(i, n, f, mid))

    def copies(j, f):
        @pl.when(j < whole)
        def _():
            among(lax.div(j, pairs), len(given), lambda a: f(a, pl.multiple_of(lax.rem(j, pairs) * 2, 2), 0, 2))

        if whole < nt:

            @pl.when(j >= whole)
            def _():
                among(j - whole, nt - whole, lambda n: [f(a, h, i, 1) for i, (a, h) in enumerate(tiles[whole + n])])

    def weights(j, slot):
        def go(a, h, i, n):
            src = given[a][0].at[:, pl.ds(pl.multiple_of(h * HEAD, HEAD), n * HEAD)]
            pltpu.make_async_copy(src, wb.at[slot, :, pl.ds(i * HEAD, n * HEAD)], wsem.at[slot]).start()

        copies(j, go)

    def sized(j, f):
        pl.when(j < nt - 1)(lambda: f(2))
        pl.when(j == nt - 1)(lambda: f(len(tiles[-1])))

    def weights_wait(j, slot):
        def go(n):
            part = wb.at[slot, :, pl.ds(0, n * HEAD)]
            pltpu.make_async_copy(part, part, wsem.at[slot]).wait()

        sized(j, go)

    def results(i):
        c, j, slot = lax.div(i, nt), lax.rem(i, nt), lax.rem(i, 2)
        here = pl.ds(pl.multiple_of(c * lump, lump), lump)

        def go(a, h, i, n):
            pltpu.make_async_copy(ob.at[slot, pl.ds(i, n)], given[a][1].at[pl.ds(h, n), :, here, :], osem.at[slot]).start()

        copies(j, go)

    def results_wait(i):
        def go(n):
            part = ob.at[lax.rem(i, 2), pl.ds(0, n)]
            pltpu.make_async_copy(part, part, osem.at[lax.rem(i, 2)]).wait()

        sized(lax.rem(i, nt), go)

    def finish(i):
        c, j, slot = lax.div(i, nt), lax.rem(i, nt), lax.rem(i, 2)
        here = pl.ds(pl.multiple_of(c * lump, lump), lump)
        turns = (j < 2 * pairs) | (j == whole) if nt > whole else j < 2 * pairs
        co, si = cos[:, here, :].reshape(m_rows, HEAD), sin[:, here, :].reshape(m_rows, HEAD)
        for n in BOTH:
            plain = acc[:, n * HEAD : (n + 1) * HEAD].astype(LOW).astype(WIDE)
            both = plain * co + pltpu.roll(plain, HALF, 1) * si
            ob[slot, n] = jnp.where(turns, both, plain).astype(LOW).reshape(owners, lump, HEAD)

    def load(c):
        return pltpu.make_async_copy(xg.at[:, pl.ds(c * lump, lump), :], xb.at[c % 2], xsem.at[c % 2])

    def actions(group):
        for what, m in group:
            if what == "send":
                message(m, True).start()
            elif what == "wait":
                message(m, False).wait_recv()
            elif what == "load":
                load(m).start()
            else:

                @pl.when(second == 0)
                def _():
                    pl.semaphore_signal(turn, 1, device_id=other, device_id_type=MESH)

    per = lump // rows

    def staged(n):
        return xb.at[1, n // per, pl.ds(n % per * rows, rows)]

    def raw(c):
        return pltpu.make_async_copy(x_ref.at[pl.ds(c * rows, rows), :], staged(c), lsem.at[c])

    def own(c):
        return pltpu.make_async_copy(staged(PIECES + c), xg.at[t, pl.ds(c * rows, rows), :], bsem.at[c])

    wide = fit(dim, 1024)

    def norm(c):
        raw(c).wait()
        src, dst = staged(c), staged(PIECES + c)

        def square(n, total):
            part = src[:, pl.ds(pl.multiple_of(n * wide, wide), wide)].astype(WIDE)
            return total + part * part

        total = lax.fori_loop(0, dim // wide, square, jnp.zeros((rows, wide), WIDE))
        scale = lax.rsqrt(jnp.sum(total, -1, keepdims=True) * (1 / dim) + EPSILON)

        def scaled(n, _):
            here = pl.ds(pl.multiple_of(n * wide, wide), wide)
            dst[:, here] = (src[:, here].astype(WIDE) * scale * gain_ref[here].astype(WIDE)[None]).astype(LOW)
            return 0

        lax.fori_loop(0, dim // wide, scaled, 0)
        own(c).start()

    for c in range(PIECES):
        raw(c).start()
    met = greet([{"tp": near} for near in (at(0, 1, 0), at(0, -1, 0), at(0, 0, 1), at(0, 0, -1))] + [other])
    weights(0, 0)
    norm(0)
    met()

    @pl.when(second == 1)
    def _():
        for c in range(1, PIECES):
            norm(c)
        pl.semaphore_wait(turn, 1)

    begins = [n for n, (what, m) in enumerate(plan[0]) if what == "send" and m[1] == 1][0]
    first = [n for n, (what, _) in enumerate(plan[0]) if what == "wait"][0]
    own(0).wait()
    actions(plan[0][:begins])

    @pl.when(second == 0)
    def _():
        norm(1)

    own(1).wait()
    actions(plan[0][begins:first])

    @pl.when(second == 0)
    def _():
        for c in range(AHEAD, PIECES):
            norm(c)

    for c in range(AHEAD, PIECES):
        own(c).wait()

    def table(n, _):
        place = (lax.broadcasted_iota(jnp.int32, (tokens, HEAD), 0) + n * tokens).astype(WIDE)
        angle = place * jnp.abs(freq_ref[...])
        cos[n] = jnp.cos(angle)
        sin[n] = jnp.sin(angle) * jnp.where(freq_ref[...] < 0, -1, 1)
        return 0

    lax.fori_loop(0, owners, table, 0)
    actions(plan[0][first:])

    def step(i, _):
        c, j, slot = lax.rem(lax.div(i, nt), 2), lax.rem(i, nt), lax.rem(i, 2)
        among(i, steps, lambda n: actions(plan[n] if n else []))

        @pl.when(i + 1 < steps)
        def _():
            weights(lax.rem(i + 1, nt), 1 - slot)

        @pl.when(j == 0)
        def _():
            pltpu.make_async_copy(xb.at[c], xb.at[c], xsem.at[c]).wait()

        weights_wait(j, slot)

        @pl.when(i > 2)
        def _():
            results_wait(i - 3)

        last = jnp.maximum(i - 1, 0)
        finish(last)
        acc[...] = dot(xb.at[c].reshape(m_rows, dim)[...], wb[slot], 1, 0)

        @pl.when(i > 0)
        def _():
            results(last)

        return 0

    acc[...] = jnp.zeros(acc.shape, acc.dtype)
    lax.fori_loop(0, steps, step, 0)
    actions(plan[-1])
    results_wait(steps - 3)
    finish(steps - 1)
    results(steps - 1)
    results_wait(steps - 2)
    results_wait(steps - 1)
    others = xg.at[pl.ds(0, owners - 1)]
    pltpu.make_async_copy(others, others, ssem).wait()


def gathered_qkv(x, gain, wq, wk, wv, owners):
    tokens, dim = x.shape
    heads = wq.shape[1] // HEAD
    freq = np.float32(THETA) ** (-np.arange(HALF, dtype=np.float32) / np.float32(HALF))
    freq = jnp.asarray(np.concatenate([-freq, freq])[None])
    lump = tokens // PIECES * LUMP
    plan = plan_gather((3 * heads + 1) // 2, 4.25)
    plan[TURN].append(("turn", None))
    out = jax.ShapeDtypeStruct((heads, owners, tokens, HEAD), LOW)
    work = 2 * owners * tokens * dim * 3 * heads * HEAD
    _, q, k, v = pl.pallas_call(
        functools.partial(gather_kernel, plan),
        out_shape=[jax.ShapeDtypeStruct((owners, tokens, dim), LOW), out, out, out],
        in_specs=[ANYWHERE, NEAR, NEAR, ANYWHERE, ANYWHERE, ANYWHERE],
        out_specs=[ANYWHERE] * 4,
        scratch_shapes=[pltpu.VMEM((2, owners, lump, dim), LOW)]
        + [pltpu.VMEM((2, dim, 2 * HEAD), LOW), pltpu.VMEM((2, 2, owners, lump, HEAD), LOW), pltpu.VMEM((owners * lump, 2 * HEAD), WIDE)]
        + [pltpu.VMEM((owners, tokens, HEAD), WIDE)] * 2
        + [DMA((PIECES,)), DMA((PIECES,)), DMA((2,)), DMA((2,)), DMA((2,)), DMA, DMA((PIECES, KINDS)), pltpu.SemaphoreType.REGULAR],
        compiler_params=pltpu.CompilerParams(collective_id=1, has_side_effects=True, vmem_limit_bytes=VMEM),
        cost_estimate=pl.CostEstimate(flops=work, transcendentals=0, bytes_accessed=dim * dim),
        name="gather_qkv",
    )(x, gain, freq, wq, wk, wv)
    whole = (heads, owners * tokens, HEAD)
    return q.reshape(whole), k.reshape(whole), v.reshape(whole)


BAND = 512
RING = 4
SUMS = 5
LATE = (0, 1, 3, 5, 7)


def scatter_kernel(seen, wo, x_ref, y_ref, a_s, w_s, t_s, s_s, h_in, f_in, h_out, f_out, hb_in, fb_in, hb_out, fb_out, x_s, y_s,
                   asem, wsem, xsem, ysem, h_r, f_r, h_t, f_t, hb_r, fb_r, hb_t, fb_t):
    heads, _, _, tokens, _ = seen.shape
    depth, dim = wo.shape
    half = BAND // 2
    bands = dim // 2 // BAND
    pos, at = place_in(lax.axis_index("tp"))
    kept = w_s.shape[1]

    def turned_by(path, d):
        return lax.rem(pos[path] + d + SIDE, SIDE)

    def columns(path, j):
        return pl.ds(pl.multiple_of(path * (dim // 2) + j * BAND, BAND), BAND)

    def near(path, last, way):
        d = 1 - 2 * way
        return at(path, d, 0) if last else at(path, 0, d)

    kinds = {"h": (h_out, h_in, h_t, h_r, False), "f": (f_out, f_in, f_t, f_r, False), "hb": (hb_out, hb_in, hb_t, hb_r, True), "fb": (fb_out, fb_in, fb_t, fb_r, True)}

    def links(kind, path, j):
        src, dst, sent, came, last = kinds[kind]
        o, i = lax.rem(j, src.shape[1]), lax.rem(j, dst.shape[1])
        return [
            pltpu.make_async_remote_copy(
                src.at[path, o, way], dst.at[path, i, way], sent.at[path, o, way], came.at[path, i, way], device_id={"tp": near(path, last, way)}, device_id_type=MESH
            )
            for way in BOTH
        ]

    def free(kind, path, j):
        @pl.when(j > 1)
        def _():
            for one in links(kind, path, j):
                one.wait_send()

    def arrived(kind, path, j):
        for one in links(kind, path, j):
            one.wait_recv()

    def post(kind, path, j):
        for one in links(kind, path, j):
            one.start()

    def term(path, n, d, j):
        b = turned_by(1 - path, d)
        rows = a_s[b] if path else a_s[:, b]
        t_s[path, n] = dot(rows.reshape(SIDE * tokens, depth), w_s[path, lax.rem(j, kept)], 1, 0).reshape(SIDE, tokens, BAND)

    def fetch_w(path, j):
        return pltpu.make_async_copy(wo.at[:, columns(path, j)], w_s.at[path, lax.rem(j, kept)], wsem.at[path, lax.rem(j, kept)])

    def fetch_x(path, j):
        return pltpu.make_async_copy(x_ref.at[:, columns(path, j)], x_s.at[path, lax.rem(j, 2)], xsem.at[path, lax.rem(j, 2)])

    def put_y(path, j):
        return pltpu.make_async_copy(y_s.at[path, lax.rem(j, 2)], y_ref.at[:, columns(path, j)], ysem.at[path, lax.rem(j, 2)])

    def part(way):
        return slice(way * half, (way + 1) * half)

    def each(f):
        lax.fori_loop(0, SIDE, lambda r, _: (f(r), 0)[1], 0)

    def slots(j):
        return lax.rem(j, 2), lax.rem(j, RING), lax.rem(j, SUMS)

    def op1(path, j):
        free("h", path, j)
        o, _, _ = slots(j)

        def add(r):
            for way in BOTH:
                h_out[path, o, way, r] = t_s[path, 0, r, :, part(way)].astype(LOW)

        each(add)
        post("h", path, j)

    def op2(path, j):
        arrived("h", path, j)
        free("f", path, j)
        o, i, _ = slots(j)

        def add(r):
            for way in BOTH:
                f_out[path, o, way, r, :, part(way)] = (t_s[path, 1 + way, r, :, part(way)] + h_in[path, i, way, r].astype(WIDE)).astype(LOW)
                f_out[path, o, way, r, :, part(1 - way)] = t_s[path, 1 + way, r, :, part(1 - way)].astype(LOW)

        each(add)
        post("f", path, j)

    def op3(path, j):
        arrived("f", path, j)
        free("hb", path, j)
        o, i, s = slots(j)

        def add(r):
            s_s[path, s, r] = t_s[path, 3, r] + f_in[path, i, 0, r].astype(WIDE) + f_in[path, i, 1, r].astype(WIDE)

        each(add)
        far = turned_by(path, 2)
        for way in BOTH:
            hb_out[path, o, way] = s_s[path, s, far, :, part(way)].astype(LOW)
        post("hb", path, j)

    def op4(path, j):
        arrived("hb", path, j)
        free("fb", path, j)
        o, i, s = slots(j)
        for way in BOTH:
            r = turned_by(path, 1 - 2 * way)
            fb_out[path, o, way, :, part(way)] = (s_s[path, s, r, :, part(way)] + hb_in[path, i, way].astype(WIDE)).astype(LOW)
            fb_out[path, o, way, :, part(1 - way)] = s_s[path, s, r, :, part(1 - way)].astype(LOW)
        post("fb", path, j)
        fetch_x(path, j).start()

    def op5(path, j):
        arrived("fb", path, j)
        fetch_x(path, j).wait()

        @pl.when(j > 1)
        def _():
            put_y(path, j).wait()

        o, i, s = slots(j)
        total = s_s[path, s, pos[path]] + fb_in[path, i, 0].astype(WIDE) + fb_in[path, i, 1].astype(WIDE)
        y_s[path, o] = (x_s[path, o].astype(WIDE) + total).astype(LOW)
        put_y(path, j).start()

    fetch_a = [pltpu.make_async_copy(seen.at[h], a_s.at[:, :, :, pl.ds(h * HEAD, HEAD)], asem.at[h]) for h in range(heads)]
    for one in fetch_a:
        one.start()
    for path in BOTH:
        fetch_w(path, 0).start()
    met = greet([{"tp": near(path, True, way)} for path in BOTH for way in BOTH])
    for one in fetch_a:
        one.wait()
    met()

    def step(i, _):
        @pl.when(i + 1 < bands)
        def _():
            for path in BOTH:
                fetch_w(path, i + 1).start()

        def run(n, f):
            j = i - LATE[n]

            @pl.when((j >= 0) & (j < bands))
            def _():
                f(j)

        def start(j):
            for path in BOTH:
                fetch_w(path, j).wait()
            for path in BOTH:
                term(path, 0, 2, j)
                op1(path, j)

        def terms(*which):
            def f(j):
                for path in BOTH:
                    for n, d in which:
                        term(path, n, d, j)

            return f

        run(0, start)
        run(1, terms((1, 1), (2, -1)))
        run(2, terms((3, 0)))
        for n, op in ((4, op5), (3, op4), (2, op3), (1, op2)):
            run(n, lambda j, op=op: [op(path, j) for path in BOTH])
        return 0

    lax.fori_loop(0, bands + LATE[-1], step, 0)
    for path in BOTH:
        for j in (bands - 2, bands - 1):
            for kind in kinds:
                for one in links(kind, path, j):
                    one.wait_send()
            put_y(path, j).wait()


def scattered(seen, wo, x):
    heads, rows, _ = seen.shape
    tokens, dim = x.shape
    depth = wo.shape[0]
    low = lambda *shape: pltpu.VMEM((2, *shape), LOW)
    wide = lambda *shape: pltpu.VMEM((2, *shape, SIDE, tokens, BAND), WIDE)
    widths = (BAND // 2, BAND)
    large = [low(n, 2, SIDE, tokens, w) for n in (RING, 2) for w in widths]
    small = [low(n, 2, tokens, w) for n in (RING, 2) for w in widths]
    sems = [DMA((2, n, 2)) for _ in BOTH for n in (RING, RING, 2, 2)]
    return pl.pallas_call(
        scatter_kernel,
        out_shape=jax.ShapeDtypeStruct((tokens, dim), LOW),
        in_specs=[ANYWHERE] * 3,
        out_specs=ANYWHERE,
        scratch_shapes=[pltpu.VMEM((SIDE, SIDE, tokens, depth), LOW), low(5, depth, BAND), wide(4), wide(SUMS)]
        + large
        + small
        + [low(2, tokens, BAND)] * 2
        + [DMA((heads,)), DMA((2, 5)), DMA((2, 2)), DMA((2, 2))]
        + sems,
        compiler_params=pltpu.CompilerParams(collective_id=2, has_side_effects=True, vmem_limit_bytes=VMEM),
        cost_estimate=pl.CostEstimate(flops=2 * rows * depth * dim, transcendentals=0, bytes_accessed=4 * depth * dim),
        name="scatter_sum",
    )(seen.reshape(heads, SIDE, SIDE, tokens, HEAD), wo, x)


def solution(mesh):
    owners = mesh.shape["tp"]

    def step(x, gain, wq, wk, wv, wo):
        q, k, v = gathered_qkv(x, gain, wq, wk, wv, owners)
        return scattered(attend(q, k, v), wo, x)

    tokens, columns = P(("dp", "tp"), None), P(None, "tp")
    return jax.shard_map(
        step,
        mesh=mesh,
        in_specs=(tokens, P(None), columns, columns, columns, P("tp", None)),
        out_specs=tokens,
        check_vma=False,
    )
```

```python
import functools
import heapq
import itertools

import jax
import jax.numpy as jnp
import numpy as np
from jax import lax
from jax.experimental import pallas as pl
from jax.experimental.pallas import tpu as pltpu
from jax.sharding import PartitionSpec as P

NEG = -1e30
HIDDEN = 2 * NEG
LOG2E = 1.4426950408889634
HEAD = 128
HALF = HEAD // 2
THETA = 10000
EPSILON = 1e-6
VMEM = 62 * 2**20
MESH = pl.DeviceIdType.MESH
ANYWHERE = pl.BlockSpec(memory_space=pl.ANY)
NEAR = pl.BlockSpec(memory_space=pltpu.VMEM)
LOW, WIDE = jnp.bfloat16, jnp.float32
DMA = pltpu.SemaphoreType.DMA
BOTH = (0, 1)


def fit(size, want):
    return max(n for n in range(HEAD, max(min(want, size), HEAD) + 1, HEAD) if size % n == 0)


def dot(a, b, ca, cb):
    return lax.dot_general(a, b, (((ca,), (cb,)), ((), ())), preferred_element_type=WIDE)


BLOCK = 512
CUTS = 4


def attention_kernel(q_ref, k_ref, v_ref, o_ref, top_s, mix_s, gap_s):
    heads, bq, d = q_ref.shape
    iq = pl.program_id(0)
    e = d**-0.5 * LOG2E
    gap_s[...] = lax.broadcasted_iota(jnp.int32, (bq, bq), 1) - lax.broadcasted_iota(jnp.int32, (bq, bq), 0)
    for h in range(heads):
        top_s[h : h + 1, :] = jnp.full((1, bq), NEG, WIDE)
        mix_s[h] = jnp.zeros(mix_s.shape[1:], WIDE)
    ones = jnp.ones((mix_s.shape[1] - d, 2 * bq), LOW)

    def block(at, size, lo, masked):
        here, qs = pl.ds(pl.multiple_of(at, HEAD), size), slice(lo, bq)
        scores = [dot(k_ref[h, here, :], q_ref[h, qs, :], 1, 1) for h in range(heads)]
        weights, keeps = [], []
        for h, s in enumerate(scores):
            if masked:
                s = jnp.where(gap_s[:size, : bq - lo] >= 0, s, HIDDEN)
            old = top_s[h : h + 1, qs]
            top = jnp.maximum(old, s.max(axis=0, keepdims=True))
            top_s[h : h + 1, qs] = top
            weights.append(jnp.exp2((s - top) * e).astype(LOW))
            keeps.append(jnp.exp2((old - top) * e))
        for h, (p, keep) in enumerate(zip(weights, keeps)):
            values = jnp.concatenate([v_ref[h, here, :].T, ones[:, :size]], axis=0)
            mix_s[h, :, qs] = mix_s[h, :, qs] * keep + dot(values, p, 1, 0)

    lax.fori_loop(0, lax.div(iq, 2), lambda j, _: block(2 * j * bq, 2 * bq, 0, False), None)
    pl.when(lax.rem(iq, 2) == 1)(lambda: block((iq - 1) * bq, bq, 0, False))
    part = bq // CUTS
    for n in range(CUTS):
        block(iq * bq + n * part, part, n * part, True)
    for h in range(heads):
        o_ref[h] = (mix_s[h, :d, :] * (1 / mix_s[h, d : d + 1, :])).T.astype(o_ref.dtype)


def attend(q, k, v):
    heads, tokens, d = q.shape
    bq = fit(tokens, BLOCK)
    some = pl.BlockSpec((heads, bq, d), lambda i: (0, i, 0))
    return pl.pallas_call(
        attention_kernel,
        grid=(tokens // bq,),
        in_specs=[some, NEAR, NEAR],
        out_specs=some,
        out_shape=jax.ShapeDtypeStruct(q.shape, q.dtype),
        scratch_shapes=[pltpu.VMEM((heads, bq), WIDE), pltpu.VMEM((heads, d + 8, bq), WIDE), pltpu.VMEM((bq, bq), jnp.int32)],
        compiler_params=pltpu.CompilerParams(dimension_semantics=("arbitrary",), vmem_limit_bytes=VMEM),
        cost_estimate=pl.CostEstimate(flops=4 * q.size * tokens, transcendentals=heads * tokens**2, bytes_accessed=8 * q.size),
        name="attention",
    )(q, k, v)


SIDE = 4
PIECES = 8
LUMP = 2
TURN = 19
AHEAD = 2
KINDS = 48


def plan_gather(tiles, tile_us):
    free, queue, done, groups, count = {}, [], [0] * PIECES, [[]], itertools.count()
    rate, delay = PIECES * 0.06, 2.5

    def send(t, m):
        stage, _, path, kind, sign, half = m
        link = (path if stage == 1 else 1 - path, sign)
        size = (1 if kind < 3 or stage == 1 else 0.5) * (0.5 if half else 1)
        free[link] = max(t, free.get(link, 0)) + size / rate
        heapq.heappush(queue, (free[link] + delay, next(count), m))
        groups[-1].append(("send", m))

    def begin(piece, t):
        for path in BOTH:
            for stage in (1, 2):
                for sign in (1, -1):
                    send(t, (stage, piece, path, 0, sign, 0))

    begun, t, tile, loaded = AHEAD, 0, 0, 0
    for n in range(AHEAD):
        begin(n, t)
    while queue or tile < tiles * PIECES // LUMP:
        while queue and queue[0][0] <= t:
            m = heapq.heappop(queue)[-1]
            groups[-1].append(("wait", m))
            stage, piece, path, kind, sign, half = m
            if stage == 1:
                if not half:
                    send(t, (1, piece, path, 0, sign, 1))
                kind = (1 if sign == 1 else 2) + 2 * half
                for way in (1, -1):
                    send(t, (2, piece, path, kind, way, 0))
            elif not half:
                send(t, (2, piece, path, kind, sign, 1))
            done[piece] += 1
            if begun < PIECES and done[begun - AHEAD] * 5 >= KINDS * 4:
                begin(begun, t)
                begun += 1
        while loaded * LUMP < PIECES and done[loaded * LUMP + LUMP - 1] == done[loaded * LUMP] == KINDS and tile >= (loaded - 1) * tiles:
            groups[-1].append(("load", loaded))
            loaded += 1
        if tile // tiles < loaded:
            groups.append([])
            tile += 1
            t += tile_us
        elif queue:
            t = max(t, queue[0][0])
    return groups


def place_in(t):
    pos = (lax.div(t, SIDE), lax.rem(t, SIDE))

    def at(path, da, db):
        a, b = lax.rem(pos[path] + da + SIDE, SIDE), lax.rem(pos[1 - path] + db + SIDE, SIDE)
        return a * SIDE + b if path == 0 else b * SIDE + a

    return pos, at


def greet(devices):
    barrier = pltpu.get_barrier_semaphore()
    for device in devices:
        pl.semaphore_signal(barrier, 1, device_id=device, device_id_type=MESH)
    return lambda: pl.semaphore_wait(barrier, len(devices))


def gather_kernel(plan, x_ref, gain_ref, freq_ref, wq, wk, wv, xg, q, k, v, xb, wb, ob, acc, cos, sin, bsem, lsem, xsem, wsem, osem, ssem, rsem, turn):
    owners, tokens, dim = xg.shape
    rows = tokens // PIECES
    lump = rows * LUMP
    m_rows = owners * lump
    split = dim // 2
    heads = q.shape[0]
    t = lax.axis_index("tp")
    pair = lax.axis_index("dp")
    second = lax.rem(pair, 2)
    other = {"dp": pair + 1 - 2 * second, "tp": t}
    _, at = place_in(t)

    def block(m, sending):
        stage, piece, path, kind, sign, half = m
        da, db, lo, width = 0, 0, 0, 4
        if stage == 1:
            da = -sign * half
            if half:
                width = 2
                lo = 1 - sign
        else:
            da, db = (0, -1, 1, 2, 2)[kind], -sign * half
            if kind > 2:
                width = 2
                lo = 2 * (kind - 3)
            if half:
                width //= 2
                lo += 0 if sign == 1 else width
        if not sending:
            da, db = (da - sign, db) if stage == 1 else (da, db - sign)
        return xg.at[at(path, da, db), pl.ds(piece * rows, rows), pl.ds(path * split + lo * split // 4, width * split // 4)]

    def message(m, sending):
        stage, piece, path, kind, sign, half = m
        key = (stage - 1) * 8 + path * 4 + kind * 8 + (sign + 1) // 2 + 2 * half
        here = block(m, sending)
        to = (at(path, sign, 0) if stage == 1 else at(path, 0, sign)) if sending else t
        return pltpu.make_async_remote_copy(here, here, ssem, rsem.at[piece, key], device_id={"tp": to}, device_id_type=MESH)

    given = ((wq, q), (wk, k), (wv, v))
    arrays = range(len(given))
    even = heads - heads % 2
    units = [(a, h) for a in arrays for h in range(even)] + [(a, h) for h in range(even, heads) for a in arrays]
    tiles = [units[n : n + 2] for n in range(0, len(units), 2)]
    nt = len(tiles)
    steps = nt * PIECES // LUMP

    pairs = even // 2
    whole = pairs * len(given)

    def among(i, n, f, first=0):
        if n - first == 1:
            f(first)
        elif n > first:
            mid = (first + n) // 2
            pl.when(i < mid)(lambda: among(i, mid, f, first))
            pl.when(i >= mid)(lambda: among(i, n, f, mid))

    def copies(j, f):
        @pl.when(j < whole)
        def _():
            among(lax.div(j, pairs), len(given), lambda a: f(a, pl.multiple_of(lax.rem(j, pairs) * 2, 2), 0, 2))

        if whole < nt:

            @pl.when(j >= whole)
            def _():
                among(j - whole, nt - whole, lambda n: [f(a, h, i, 1) for i, (a, h) in enumerate(tiles[whole + n])])

    def weights(j, slot):
        def go(a, h, i, n):
            src = given[a][0].at[:, pl.ds(pl.multiple_of(h * HEAD, HEAD), n * HEAD)]
            pltpu.make_async_copy(src, wb.at[slot, :, pl.ds(i * HEAD, n * HEAD)], wsem.at[slot]).start()

        copies(j, go)

    def sized(j, f):
        pl.when(j < nt - 1)(lambda: f(2))
        pl.when(j == nt - 1)(lambda: f(len(tiles[-1])))

    def weights_wait(j, slot):
        def go(n):
            part = wb.at[slot, :, pl.ds(0, n * HEAD)]
            pltpu.make_async_copy(part, part, wsem.at[slot]).wait()

        sized(j, go)

    def results(i):
        c, j, slot = lax.div(i, nt), lax.rem(i, nt), lax.rem(i, 2)
        here = pl.ds(pl.multiple_of(c * lump, lump), lump)

        def go(a, h, i, n):
            pltpu.make_async_copy(ob.at[slot, pl.ds(i, n)], given[a][1].at[pl.ds(h, n), :, here, :], osem.at[slot]).start()

        copies(j, go)

    def results_wait(i):
        def go(n):
            part = ob.at[lax.rem(i, 2), pl.ds(0, n)]
            pltpu.make_async_copy(part, part, osem.at[lax.rem(i, 2)]).wait()

        sized(lax.rem(i, nt), go)

    def finish(i):
        c, j, slot = lax.div(i, nt), lax.rem(i, nt), lax.rem(i, 2)
        here = pl.ds(pl.multiple_of(c * lump, lump), lump)
        turns = (j < 2 * pairs) | (j == whole) if nt > whole else j < 2 * pairs
        co, si = cos[:, here, :].reshape(m_rows, HEAD), sin[:, here, :].reshape(m_rows, HEAD)
        for n in BOTH:
            plain = acc[:, n * HEAD : (n + 1) * HEAD].astype(LOW).astype(WIDE)
            both = plain * co + pltpu.roll(plain, HALF, 1) * si
            ob[slot, n] = jnp.where(turns, both, plain).astype(LOW).reshape(owners, lump, HEAD)

    def load(c):
        return pltpu.make_async_copy(xg.at[:, pl.ds(c * lump, lump), :], xb.at[c % 2], xsem.at[c % 2])

    def actions(group):
        for what, m in group:
            if what == "send":
                message(m, True).start()
            elif what == "wait":
                message(m, False).wait_recv()
            elif what == "load":
                load(m).start()
            else:

                @pl.when(second == 0)
                def _():
                    pl.semaphore_signal(turn, 1, device_id=other, device_id_type=MESH)

    per = lump // rows

    def staged(n):
        return xb.at[1, n // per, pl.ds(n % per * rows, rows)]

    def raw(c):
        return pltpu.make_async_copy(x_ref.at[pl.ds(c * rows, rows), :], staged(c), lsem.at[c])

    def own(c):
        return pltpu.make_async_copy(staged(PIECES + c), xg.at[t, pl.ds(c * rows, rows), :], bsem.at[c])

    wide = fit(dim, 1024)

    def norm(c):
        raw(c).wait()
        src, dst = staged(c), staged(PIECES + c)

        def square(n, total):
            part = src[:, pl.ds(pl.multiple_of(n * wide, wide), wide)].astype(WIDE)
            return total + part * part

        total = lax.fori_loop(0, dim // wide, square, jnp.zeros((rows, wide), WIDE))
        scale = lax.rsqrt(jnp.sum(total, -1, keepdims=True) * (1 / dim) + EPSILON)

        def scaled(n, _):
            here = pl.ds(pl.multiple_of(n * wide, wide), wide)
            dst[:, here] = (src[:, here].astype(WIDE) * scale * gain_ref[here].astype(WIDE)[None]).astype(LOW)
            return 0

        lax.fori_loop(0, dim // wide, scaled, 0)
        own(c).start()

    for c in range(PIECES):
        raw(c).start()
    met = greet([{"tp": near} for near in (at(0, 1, 0), at(0, -1, 0), at(0, 0, 1), at(0, 0, -1))] + [other])
    weights(0, 0)
    norm(0)
    met()

    @pl.when(second == 1)
    def _():
        for c in range(1, PIECES):
            norm(c)
        pl.semaphore_wait(turn, 1)

    begins = [n for n, (what, m) in enumerate(plan[0]) if what == "send" and m[1] == 1][0]
    first = [n for n, (what, _) in enumerate(plan[0]) if what == "wait"][0]
    own(0).wait()
    actions(plan[0][:begins])

    @pl.when(second == 0)
    def _():
        norm(1)

    own(1).wait()
    actions(plan[0][begins:first])

    @pl.when(second == 0)
    def _():
        for c in range(AHEAD, PIECES):
            norm(c)

    for c in range(AHEAD, PIECES):
        own(c).wait()

    def table(n, _):
        place = (lax.broadcasted_iota(jnp.int32, (tokens, HEAD), 0) + n * tokens).astype(WIDE)
        angle = place * jnp.abs(freq_ref[...])
        cos[n] = jnp.cos(angle)
        sin[n] = jnp.sin(angle) * jnp.where(freq_ref[...] < 0, -1, 1)
        return 0

    lax.fori_loop(0, owners, table, 0)
    actions(plan[0][first:])

    def step(i, _):
        c, j, slot = lax.rem(lax.div(i, nt), 2), lax.rem(i, nt), lax.rem(i, 2)
        among(i, steps, lambda n: actions(plan[n] if n else []))

        @pl.when(i + 1 < steps)
        def _():
            weights(lax.rem(i + 1, nt), 1 - slot)

        @pl.when(j == 0)
        def _():
            pltpu.make_async_copy(xb.at[c], xb.at[c], xsem.at[c]).wait()

        weights_wait(j, slot)

        @pl.when(i > 2)
        def _():
            results_wait(i - 3)

        last = jnp.maximum(i - 1, 0)
        finish(last)
        acc[...] = dot(xb.at[c].reshape(m_rows, dim)[...], wb[slot], 1, 0)

        @pl.when(i > 0)
        def _():
            results(last)

        return 0

    acc[...] = jnp.zeros(acc.shape, acc.dtype)
    lax.fori_loop(0, steps, step, 0)
    actions(plan[-1])
    results_wait(steps - 3)
    finish(steps - 1)
    results(steps - 1)
    results_wait(steps - 2)
    results_wait(steps - 1)
    others = xg.at[pl.ds(0, owners - 1)]
    pltpu.make_async_copy(others, others, ssem).wait()


def gathered_qkv(x, gain, wq, wk, wv, owners):
    tokens, dim = x.shape
    heads = wq.shape[1] // HEAD
    freq = np.float32(THETA) ** (-np.arange(HALF, dtype=np.float32) / np.float32(HALF))
    freq = jnp.asarray(np.concatenate([-freq, freq])[None])
    lump = tokens // PIECES * LUMP
    plan = plan_gather((3 * heads + 1) // 2, 4.25)
    plan[TURN].append(("turn", None))
    out = jax.ShapeDtypeStruct((heads, owners, tokens, HEAD), LOW)
    work = 2 * owners * tokens * dim * 3 * heads * HEAD
    _, q, k, v = pl.pallas_call(
        functools.partial(gather_kernel, plan),
        out_shape=[jax.ShapeDtypeStruct((owners, tokens, dim), LOW), out, out, out],
        in_specs=[ANYWHERE, NEAR, NEAR, ANYWHERE, ANYWHERE, ANYWHERE],
        out_specs=[ANYWHERE] * 4,
        scratch_shapes=[pltpu.VMEM((2, owners, lump, dim), LOW)]
        + [pltpu.VMEM((2, dim, 2 * HEAD), LOW), pltpu.VMEM((2, 2, owners, lump, HEAD), LOW), pltpu.VMEM((owners * lump, 2 * HEAD), WIDE)]
        + [pltpu.VMEM((owners, tokens, HEAD), WIDE)] * 2
        + [DMA((PIECES,)), DMA((PIECES,)), DMA((2,)), DMA((2,)), DMA((2,)), DMA, DMA((PIECES, KINDS)), pltpu.SemaphoreType.REGULAR],
        compiler_params=pltpu.CompilerParams(collective_id=1, has_side_effects=True, vmem_limit_bytes=VMEM),
        cost_estimate=pl.CostEstimate(flops=work, transcendentals=0, bytes_accessed=dim * dim),
        name="gather_qkv",
    )(x, gain, freq, wq, wk, wv)
    whole = (heads, owners * tokens, HEAD)
    return q.reshape(whole), k.reshape(whole), v.reshape(whole)


BAND = 512
RING = 4
SUMS = 5
LATE = (0, 1, 3, 5, 7)


def scatter_kernel(seen, wo, x_ref, y_ref, a_s, w_s, t_s, s_s, h_in, f_in, h_out, f_out, hb_in, fb_in, hb_out, fb_out, x_s, y_s,
                   asem, wsem, xsem, ysem, h_r, f_r, h_t, f_t, hb_r, fb_r, hb_t, fb_t):
    heads, _, _, tokens, _ = seen.shape
    depth, dim = wo.shape
    half = BAND // 2
    bands = dim // 2 // BAND
    pos, at = place_in(lax.axis_index("tp"))
    kept = w_s.shape[1]

    def turned_by(path, d):
        return lax.rem(pos[path] + d + SIDE, SIDE)

    def columns(path, j):
        return pl.ds(pl.multiple_of(path * (dim // 2) + j * BAND, BAND), BAND)

    def near(path, last, way):
        d = 1 - 2 * way
        return at(path, d, 0) if last else at(path, 0, d)

    kinds = {"h": (h_out, h_in, h_t, h_r, False), "f": (f_out, f_in, f_t, f_r, False), "hb": (hb_out, hb_in, hb_t, hb_r, True), "fb": (fb_out, fb_in, fb_t, fb_r, True)}

    def links(kind, path, j):
        src, dst, sent, came, last = kinds[kind]
        o, i = lax.rem(j, src.shape[1]), lax.rem(j, dst.shape[1])
        return [
            pltpu.make_async_remote_copy(
                src.at[path, o, way], dst.at[path, i, way], sent.at[path, o, way], came.at[path, i, way], device_id={"tp": near(path, last, way)}, device_id_type=MESH
            )
            for way in BOTH
        ]

    def free(kind, path, j):
        @pl.when(j > 1)
        def _():
            for one in links(kind, path, j):
                one.wait_send()

    def arrived(kind, path, j):
        for one in links(kind, path, j):
            one.wait_recv()

    def post(kind, path, j):
        for one in links(kind, path, j):
            one.start()

    def term(path, n, d, j):
        b = turned_by(1 - path, d)
        rows = a_s[b] if path else a_s[:, b]
        t_s[path, n] = dot(rows.reshape(SIDE * tokens, depth), w_s[path, lax.rem(j, kept)], 1, 0).reshape(SIDE, tokens, BAND)

    def fetch_w(path, j):
        return pltpu.make_async_copy(wo.at[:, columns(path, j)], w_s.at[path, lax.rem(j, kept)], wsem.at[path, lax.rem(j, kept)])

    def fetch_x(path, j):
        return pltpu.make_async_copy(x_ref.at[:, columns(path, j)], x_s.at[path, lax.rem(j, 2)], xsem.at[path, lax.rem(j, 2)])

    def put_y(path, j):
        return pltpu.make_async_copy(y_s.at[path, lax.rem(j, 2)], y_ref.at[:, columns(path, j)], ysem.at[path, lax.rem(j, 2)])

    def part(way):
        return slice(way * half, (way + 1) * half)

    def each(f):
        lax.fori_loop(0, SIDE, lambda r, _: (f(r), 0)[1], 0)

    def slots(j):
        return lax.rem(j, 2), lax.rem(j, RING), lax.rem(j, SUMS)

    def op1(path, j):
        free("h", path, j)
        o, _, _ = slots(j)

        def add(r):
            for way in BOTH:
                h_out[path, o, way, r] = t_s[path, 0, r, :, part(way)].astype(LOW)

        each(add)
        post("h", path, j)

    def op2(path, j):
        arrived("h", path, j)
        free("f", path, j)
        o, i, _ = slots(j)

        def add(r):
            for way in BOTH:
                f_out[path, o, way, r, :, part(way)] = (t_s[path, 1 + way, r, :, part(way)] + h_in[path, i, way, r].astype(WIDE)).astype(LOW)
                f_out[path, o, way, r, :, part(1 - way)] = t_s[path, 1 + way, r, :, part(1 - way)].astype(LOW)

        each(add)
        post("f", path, j)

    def op3(path, j):
        arrived("f", path, j)
        free("hb", path, j)
        o, i, s = slots(j)

        def add(r):
            s_s[path, s, r] = t_s[path, 3, r] + f_in[path, i, 0, r].astype(WIDE) + f_in[path, i, 1, r].astype(WIDE)

        each(add)
        far = turned_by(path, 2)
        for way in BOTH:
            hb_out[path, o, way] = s_s[path, s, far, :, part(way)].astype(LOW)
        post("hb", path, j)

    def op4(path, j):
        arrived("hb", path, j)
        free("fb", path, j)
        o, i, s = slots(j)
        for way in BOTH:
            r = turned_by(path, 1 - 2 * way)
            fb_out[path, o, way, :, part(way)] = (s_s[path, s, r, :, part(way)] + hb_in[path, i, way].astype(WIDE)).astype(LOW)
            fb_out[path, o, way, :, part(1 - way)] = s_s[path, s, r, :, part(1 - way)].astype(LOW)
        post("fb", path, j)
        fetch_x(path, j).start()

    def op5(path, j):
        arrived("fb", path, j)
        fetch_x(path, j).wait()

        @pl.when(j > 1)
        def _():
            put_y(path, j).wait()

        o, i, s = slots(j)
        total = s_s[path, s, pos[path]] + fb_in[path, i, 0].astype(WIDE) + fb_in[path, i, 1].astype(WIDE)
        y_s[path, o] = (x_s[path, o].astype(WIDE) + total).astype(LOW)
        put_y(path, j).start()

    fetch_a = [pltpu.make_async_copy(seen.at[h], a_s.at[:, :, :, pl.ds(h * HEAD, HEAD)], asem.at[h]) for h in range(heads)]
    for one in fetch_a:
        one.start()
    for path in BOTH:
        fetch_w(path, 0).start()
    met = greet([{"tp": near(path, True, way)} for path in BOTH for way in BOTH])
    for one in fetch_a:
        one.wait()
    met()

    def step(i, _):
        @pl.when(i + 1 < bands)
        def _():
            for path in BOTH:
                fetch_w(path, i + 1).start()

        def run(n, f):
            j = i - LATE[n]

            @pl.when((j >= 0) & (j < bands))
            def _():
                f(j)

        def start(j):
            for path in BOTH:
                fetch_w(path, j).wait()
            for path in BOTH:
                term(path, 0, 2, j)
                op1(path, j)

        def terms(*which):
            def f(j):
                for path in BOTH:
                    for n, d in which:
                        term(path, n, d, j)

            return f

        run(0, start)
        run(1, terms((1, 1), (2, -1)))
        run(2, terms((3, 0)))
        for n, op in ((4, op5), (3, op4), (2, op3), (1, op2)):
            run(n, lambda j, op=op: [op(path, j) for path in BOTH])
        return 0

    lax.fori_loop(0, bands + LATE[-1], step, 0)
    for path in BOTH:
        for j in (bands - 2, bands - 1):
            for kind in kinds:
                for one in links(kind, path, j):
                    one.wait_send()
            put_y(path, j).wait()


def scattered(seen, wo, x):
    heads, rows, _ = seen.shape
    tokens, dim = x.shape
    depth = wo.shape[0]
    low = lambda *shape: pltpu.VMEM((2, *shape), LOW)
    wide = lambda *shape: pltpu.VMEM((2, *shape, SIDE, tokens, BAND), WIDE)
    widths = (BAND // 2, BAND)
    large = [low(n, 2, SIDE, tokens, w) for n in (RING, 2) for w in widths]
    small = [low(n, 2, tokens, w) for n in (RING, 2) for w in widths]
    sems = [DMA((2, n, 2)) for _ in BOTH for n in (RING, RING, 2, 2)]
    return pl.pallas_call(
        scatter_kernel,
        out_shape=jax.ShapeDtypeStruct((tokens, dim), LOW),
        in_specs=[ANYWHERE] * 3,
        out_specs=ANYWHERE,
        scratch_shapes=[pltpu.VMEM((SIDE, SIDE, tokens, depth), LOW), low(5, depth, BAND), wide(4), wide(SUMS)]
        + large
        + small
        + [low(2, tokens, BAND)] * 2
        + [DMA((heads,)), DMA((2, 5)), DMA((2, 2)), DMA((2, 2))]
        + sems,
        compiler_params=pltpu.CompilerParams(collective_id=2, has_side_effects=True, vmem_limit_bytes=VMEM),
        cost_estimate=pl.CostEstimate(flops=2 * rows * depth * dim, transcendentals=0, bytes_accessed=4 * depth * dim),
        name="scatter_sum",
    )(seen.reshape(heads, SIDE, SIDE, tokens, HEAD), wo, x)


def handed_on(y):
    rows = y.shape[0] // SIDE

    def kernel(src, dst):
        dst[...] = src[...]

    block = pl.BlockSpec((rows, y.shape[1]), lambda i: (i, 0))
    return pl.pallas_call(kernel, grid=(SIDE,), in_specs=[block], out_specs=block, out_shape=jax.ShapeDtypeStruct(y.shape, y.dtype), name="handed_on")(y)


def solution(mesh):
    owners = mesh.shape["tp"]

    def step(x, gain, wq, wk, wv, wo):
        q, k, v = gathered_qkv(x, gain, wq, wk, wv, owners)
        return handed_on(scattered(attend(q, k, v), wo, x))

    tokens, columns = P(("dp", "tp"), None), P(None, "tp")
    return jax.shard_map(
        step,
        mesh=mesh,
        in_specs=(tokens, P(None), columns, columns, columns, P("tp", None)),
        out_specs=tokens,
        check_vma=False,
    )
```
